32 devices in a mesh: groups: 2 (over x), row: 8 (over z, y), col: 2 (over core).
Axes of the slice: x: 2, y: 2, z: 4, core: 2. Of those that a mesh axis runs over, the one named last changes fastest.
Arguments:
- inverse: float32 [16, 2, 128, 2048], P('groups', 'col', None, 'row'), parts along dimension 0, as said below
- features: float32 [16384, 1024], P(('groups', 'row')), parts along dimension 0, may hold values from -6 to 6
- residual: float32 [16384, 256], P(('groups', 'row')), parts along dimension 0, may hold values from -6 to 6
- block_ids: int32 [4096], P(('groups', 'row')), parts along dimension 0, may hold values from 0 to 8191, as said below
Outputs:
- updated: float32 [16384, 256], P(('groups', 'row'), 'col'), parts along dimension 0
The draws below stay inside these ranges and needn't reach their ends.
There are 2 independent parts, one for each index of `groups`. The reference program is written for one: setup_inputs(seed, part) draws one part's arguments, and reference() takes and returns one part's arrays. A program takes and returns all parts, laid end to end along the dimension named above; each array names one. Nothing has to cross between parts.
Inputs may be any that keep to these rules, and one draw needn't show every extreme that they name: `block_ids`: the ids at block positions a * 256 to (a + 1) * 256 - 1 are distinct and lie in a * 1024 to (a + 1) * 1024 - 1. `inverse`: read as a [2048, 2048] matrix, each row is a positive scale between 0.3 and 3.4 times an identity row plus small independent entries.
All inputs are finite; a program needn't handle non-finite values.
Results may differ from the reference program's by a relative error of at most 0.000084.
Values sent between devices are 32-bit elements; how exact they have to be, the bound alone decides.
A program may use at most 128 MiB of HBM per device.

```python
import jax
import jax.numpy as jnp
from jax import lax

F = 1024
R = 256
BLK_DEV = 256
ROWS_DEV = 1024
HALF = 128
B = 2048
M = 8192


def draw_inverse(key, part):
    scale = 0.6 / B ** 0.5
    entries = jax.random.normal(jax.random.fold_in(key, 13), (B, B), jnp.float32)
    full = entries * scale + jnp.eye(B, dtype=jnp.float32)
    return full.reshape(B // BLK_DEV, BLK_DEV // HALF, HALF, B)


def draw_block_ids(key, part):
    groups_count = B // BLK_DEV
    keys = jax.random.split(jax.random.fold_in(key, 21), groups_count)
    picked = jax.vmap(lambda k: jax.random.permutation(k, ROWS_DEV)[:BLK_DEV])(keys)
    offsets = (jnp.arange(groups_count, dtype=jnp.int32) * ROWS_DEV)[:, None]
    return (picked.astype(jnp.int32) + offsets).reshape(B)


def shard_levels(rng, dims, cuts, least, high):
    level, own = 1.0, jax.random.fold_in(rng, 6)
    for position, parts in cuts:
        draws = jnp.exp(jax.random.uniform(jax.random.fold_in(own, position), (parts,), jnp.float32, least / len(cuts), high / len(cuts)))
        level = level * jnp.repeat(draws, dims[position] // parts).reshape([-1 if axis == position else 1 for axis in range(len(dims))])
    return level


def gaussian(own_key, dims, deviation, most, cuts=(), kind=jnp.bfloat16):
    result = deviation * jax.random.normal(own_key, dims, jnp.float32)
    if cuts:
        result = result * shard_levels(own_key, dims, cuts, -0.22, 0.18)
    return jnp.clip(result, -most, most).astype(kind)


def setup_inputs(seed: int = 0, part: int = 0) -> dict:
    seeds = jax.random.split(jax.random.key(seed), 5)
    part_splits = jax.random.split(jax.random.fold_in(seeds[4], part), 5)
    inverse = draw_inverse(jax.random.fold_in(jax.random.fold_in(seeds[4], part), 71), part)
    features = gaussian(part_splits[1], (M, F), 1.0, 6.0, ((0, 8),), jnp.float32)
    residual = gaussian(part_splits[2], (M, R), 1.0, 6.0, ((0, 8),), jnp.float32)
    block_ids = draw_block_ids(jax.random.fold_in(jax.random.fold_in(seeds[4], part), 71), part)
    return {"inverse": inverse, "features": features, "residual": residual, "block_ids": block_ids}


def kernel_rows(rows_x, block_x, correction):
    gram = jnp.dot(rows_x, block_x.T, precision=lax.Precision.HIGHEST, preferred_element_type=jnp.float32)
    kern = (gram / F + 0.5) ** 2
    return jnp.dot(kern, correction, precision=lax.Precision.HIGHEST, preferred_element_type=jnp.float32)


def reference(inverse, features, residual, block_ids):
    inv = inverse.reshape(B, B)
    block_res = jnp.take(residual, block_ids, axis=0)
    correction = jnp.dot(inv, block_res, precision=lax.Precision.HIGHEST, preferred_element_type=jnp.float32)
    block_x = jnp.take(features, block_ids, axis=0)
    blocks = features.reshape(M // ROWS_DEV, ROWS_DEV, F)
    change = lax.map(lambda rows_x: kernel_rows(rows_x, block_x, correction), blocks)
    return residual - change.reshape(M, R)
```

```python
import functools

import jax
import jax.numpy as jnp
from jax import lax
from jax.experimental import pallas as pl
from jax.experimental.pallas import tpu as pltpu
from jax.sharding import PartitionSpec as P

F32, BF16 = jnp.float32, jnp.bfloat16
MESH = pl.DeviceIdType.MESH
NN = (((1,), (0,)), ((), ()))
NT = (((1,), (1,)), ((), ()))


def split(v):
    hi = v.astype(BF16)
    return hi, (v - hi.astype(F32)).astype(BF16)


def dot3(a, b, dims):
    def one(x, y):
        return lax.dot_general(x, y, dims, preferred_element_type=F32)

    return one(a[0], b[1]) + one(a[1], b[0]) + one(a[0], b[0])


def ring_kernel(
    n, snake, ids, feat_hbm, res_hbm, inv_hbm, out, feat, fhi, flo, res, inv, bres, xh, xl, xbuf,
    kbuf, cbuf, rbuf, change, ebuf, lsem, xs_sem, xr_sem, ss_sem, sr_sem, es_sem, er_sem,
):
    me, core = lax.axis_index("row"), lax.axis_index("col")
    half_n = n // 2
    rows, feats = feat.shape
    blk = ids.shape[0]
    half = blk // 2
    quarter = half // 2
    width = out.shape[1]
    slots = kbuf.shape[0]
    tile = min(512, rows)

    def pos_of(r):
        if not snake:
            return r
        z, y = r // 2, r % 2
        return (1 - y) * z + y * (n - 1 - z)

    def row_of(p):
        p = lax.rem(p + n, n)
        if not snake:
            return p
        q = p // half_n
        return (1 - q) * 2 * p + q * (2 * (n - 1 - p) + 1)

    pos = pos_of(me)
    ahead = (row_of(pos + 1), row_of(pos + n - 1))
    sign = (1, -1)

    loads = [
        pltpu.make_async_copy(feat_hbm, feat, lsem.at[0]),
        pltpu.make_async_copy(res_hbm, res, lsem.at[1]),
        pltpu.make_async_copy(inv_hbm, inv, lsem.at[2]),
    ]
    for load in loads:
        load.start()
    barrier = pltpu.get_barrier_semaphore()
    for target in ({"row": ahead[0]}, {"row": ahead[1]}, {"col": 1 - core}):
        pl.semaphore_signal(barrier, inc=1, device_id=target, device_id_type=MESH)

    def remote(src, dst, send, recv, target):
        return pltpu.make_async_remote_copy(
            src_ref=src, dst_ref=dst, send_sem=send, recv_sem=recv, device_id=target,
            device_id_type=MESH,
        )

    def x_copy(way, p):
        d, h = p // 2 + 1, (p + way) % 2
        src = way * half + h * quarter
        dst = way * quarter if d == half_n else src
        return remote(
            xbuf.at[d - 1, pl.ds(src, quarter)], xbuf.at[d, pl.ds(dst, quarter)],
            xs_sem.at[way, p], xr_sem.at[way, p], {"row": ahead[way]},
        )

    def small_copy(way, m):
        if m <= half_n:
            at = pl.ds(way * quarter, quarter) if m == 1 else pl.ds(0, half)
            src, dst = rbuf.at[way, m - 1, at], rbuf.at[way, m, at]
        else:
            s = m - half_n
            if s == half_n:
                src = cbuf.at[s - 1, pl.ds(way * half + way * quarter, quarter)]
                dst = cbuf.at[s, pl.ds(way * quarter, quarter)]
            else:
                src = cbuf.at[s - 1, pl.ds(way * half, half)]
                dst = cbuf.at[s, pl.ds(way * half, half)]
        return remote(
            src, dst, ss_sem.at[way, m - 1], sr_sem.at[way, m - 1], {"row": ahead[way]}
        )

    def partial_value(owner, at=None):
        a = inv[owner, 0] if at is None else inv[owner, 0, at]
        return dot3(split(a), (bres[0], bres[1]), NN)

    def gram(d, cols):
        hi, lo = split(xbuf[d, pl.ds(0, cols)])
        xh[pl.ds(0, cols)] = hi
        xl[pl.ds(0, cols)] = lo

        def body(i, _):
            at = pl.ds(pl.multiple_of(i * tile, tile), tile)
            g = dot3((fhi[at], flo[at]), (xh[pl.ds(0, cols)], xl[pl.ds(0, cols)]), NT)
            g = g * (1.0 / feats) + 0.5
            kbuf[d % slots, at, pl.ds(0, cols)] = g * g
            return 0

        lax.fori_loop(0, rows // tile, body, 0)

    def apply(d, cols):
        c = split(cbuf[d, pl.ds(0, cols)])

        def body(i, _):
            at = pl.ds(pl.multiple_of(i * tile, tile), tile)
            add = dot3(split(kbuf[d % slots, at, pl.ds(0, cols)]), c, NN)
            change[at] = add if d == 0 else change[at] + add
            return 0

        lax.fori_loop(0, rows // tile, body, 0)

    base = me * rows

    def local(i):
        return jnp.maximum(jnp.minimum(ids[i] - base, rows - 1), 0)

    loads[0].wait()

    def gather_x(i, _):
        v = feat[pl.ds(local(core * half + i), 1), :]
        xbuf[0, pl.ds(i, 1), :] = v
        xbuf[0, pl.ds(half + i, 1), :] = v
        return 0

    lax.fori_loop(0, half, gather_x, 0, unroll=8)
    pl.semaphore_wait(barrier, 3)
    for way in (0, 1):
        x_copy(way, 0).start()

    loads[1].wait()

    def gather_res(i, _):
        change[pl.ds(i, 1), :] = res[pl.ds(local(i), 1), :]
        return 0

    lax.fori_loop(0, blk, gather_res, 0, unroll=8)
    hi, lo = split(change[pl.ds(0, blk)])
    bres[0] = hi
    bres[1] = lo
    loads[2].wait()
    for way in (0, 1):
        at = pl.ds(way * quarter, quarter)
        rbuf[way, 0, at] = partial_value(row_of(pos + half_n), at)
        small_copy(way, 1).start()

    def split_feat(i, _):
        at = pl.ds(pl.multiple_of(i * quarter, quarter), quarter)
        hi, lo = split(feat[at])
        fhi[at] = hi
        flo[at] = lo
        return 0

    lax.fori_loop(0, rows // quarter, split_feat, 0)
    for k in range(n):
        m = k + 1
        for way in (0, 1):
            small_copy(way, m).wait_recv()
            if m < half_n:
                part = partial_value(row_of(pos + n + sign[way] * (half_n - m)))
                if m == 1:
                    got, other = pl.ds(way * quarter, quarter), (1 - way) * quarter
                    lo_part, hi_part = part[:quarter], part[quarter:]
                    mine, rest = (lo_part, hi_part) if way == 0 else (hi_part, lo_part)
                    rbuf[way, 1, got] = rbuf[way, 1, got] + mine
                    rbuf[way, 1, pl.ds(other, quarter)] = rest
                else:
                    rbuf[way, m] = rbuf[way, m] + part
            elif m == half_n and way == 1:
                corr = partial_value(me) + rbuf[0, half_n] + rbuf[1, half_n]
                cbuf[0, pl.ds(0, half)] = corr
                cbuf[0, pl.ds(half, half)] = corr
                small_copy(0, m + 1).start()
            if m < n and (m != half_n or way == 1):
                small_copy(way, m + 1).start()
            if k >= 1:
                x_copy(way, k - 1).wait_recv()
            if k + 1 <= n - 2:
                x_copy(way, k + 1).start()
        if k == 0:
            gram(0, half)
        if k % 2 == 0 and k >= 2:
            gram(k // 2, blk)
        if k == half_n - 1:
            apply(0, half)
        if half_n <= k < n - 1:
            apply(k - half_n + 1, blk)

    gram(half_n, half)
    c = split(cbuf[half_n, pl.ds(0, half)])
    mine = pl.ds(pl.multiple_of(core * width, width), width)
    theirs = pl.ds(pl.multiple_of((1 - core) * width, width), width)
    step = tile // 2

    def swap(i):
        at = pl.ds(i * step, step)
        return remote(
            change.at[at, theirs], ebuf.at[at, pl.ds(0, width)], es_sem.at[i], er_sem.at[i],
            {"col": 1 - core},
        )

    for i in range(rows // step):
        at = pl.ds(i * step, step)
        change[at] += dot3(split(kbuf[half_n % slots, at, pl.ds(0, half)]), c, NN)
        swap(i).start()
    for i in range(rows // step):
        at = pl.ds(i * step, step)
        swap(i).wait_recv()
        out[at] = res[at, mine] - (change[at, mine] + ebuf[at, pl.ds(0, width)])
    for way in (0, 1):
        for p in range(n - 1):
            x_copy(way, p).wait_send()
        for m in range(1, n + 1):
            small_copy(way, m).wait_send()
    for i in range(rows // step):
        swap(i).wait_send()


def ring(snake, inverse, features, residual, block_ids):
    n, cores = lax.axis_size("row"), lax.axis_size("col")
    rows, feats = features.shape
    rhs = residual.shape[1]
    blk = block_ids.shape[0]
    half, half_n = blk // cores, n // 2
    any_spec = pl.BlockSpec(memory_space=pl.ANY)
    dma = pltpu.SemaphoreType.DMA
    tiles = rows // (min(512, rows) // 2)
    return pl.pallas_call(
        functools.partial(ring_kernel, n, snake),
        out_shape=jax.ShapeDtypeStruct((rows, rhs // cores), F32),
        in_specs=[pl.BlockSpec(memory_space=pltpu.SMEM), any_spec, any_spec, any_spec],
        out_specs=pl.BlockSpec(memory_space=pltpu.VMEM),
        scratch_shapes=[
            pltpu.VMEM((rows, feats), F32),
            pltpu.VMEM((rows, feats), BF16),
            pltpu.VMEM((rows, feats), BF16),
            pltpu.VMEM((rows, rhs), F32),
            pltpu.VMEM(inverse.shape, F32),
            pltpu.VMEM((2, blk, rhs), BF16),
            pltpu.VMEM((blk, feats), BF16),
            pltpu.VMEM((blk, feats), BF16),
            pltpu.VMEM((half_n + 1, blk, feats), F32),
            pltpu.VMEM((n // 4 + 2, rows, blk), F32),
            pltpu.VMEM((half_n + 1, blk, rhs), F32),
            pltpu.VMEM((2, half_n + 1, half, rhs), F32),
            pltpu.VMEM((rows, rhs), F32),
            pltpu.VMEM((rows, rhs), F32),
            dma((3,)),
            dma((2, n - 1)),
            dma((2, n - 1)),
            dma((2, n)),
            dma((2, n)),
            dma((tiles,)),
            dma((tiles,)),
        ],
        compiler_params=pltpu.CompilerParams(
            collective_id=0, has_side_effects=True, vmem_limit_bytes=67043328
        ),
    )(block_ids, features, residual, inverse)


CORNER_Z = (
    "Xa0", "Xa1", "Rf", "Rd", "Rh", "Rb", "Xa2", "Xa3", "Rg", "Re", "Ra", "Rc",
    "Xb0", "Xb1", "Xb2", "Xb3",
)
CORNER_Y = (
    "Xa0", "Xa2", "Xa3", "Xa1", "Xc0", "Xc1", "Xc2", "Xc3", "Xe0", "Xg0", "Xe1", "Xg1",
    "Xg2", "Xg3", "Xe2", "Xe3", "Cg", "Ce",
)
INNER_Z = (
    "Xc0", "Xc1", "Xc2", "Xc3", "Xe2", "Xe3", "Xe0", "Xg0", "Xe1", "Xg1", "Xg2", "Xg3",
    "Ca", "Cc", "Cg", "Ce", "Cb", "Cd",
)
INNER_W = (
    "Xc0", "Xc2", "Xc3", "Xc1", "Sf", "Xa0", "Sh", "Xa1", "Xa2", "Xa3", "Sg", "Se", "Ca", "Cc",
)
INNER_Y = (
    "Xc0", "Xc1", "Xc2", "Xe2", "Xe3", "Xc3", "Td", "Xg0", "Tb", "Xg1", "Xg2", "Xg3",
    "Ca", "Cc", "Xe0", "Xe1", "Cg", "Ce",
)
OVER_Y = dict(zip("abcdefgh", "badcfehg"))
OVER_Z = dict(zip("abcdefgh", "ghefcdab"))


def seen(order, swap):
    return [i[0] + swap.get(i[1], i[1]) + i[2:] for i in order]


def slots(*links):
    most = max(len(link) for link in links)
    return [[link[k] for link in links if k < len(link)] for k in range(most)]


def mesh_kernel(
    ids, feat_hbm, res_hbm, inv_hbm, out, feat, fhi, flo, res, inv, bres, xall, xh, xl, khi, klo,
    call, chi, clo, own, part, half_sum, col_sum, change, ebuf, lsem, xs, xr, cs, cr, rs, rr, ss,
    sr, ts, tr, es, er,
):
    me, core = lax.axis_index("row"), lax.axis_index("col")
    rows, feats = feat.shape
    blk = ids.shape[0]
    half = blk // 2
    quarter = half // 4
    width = out.shape[1]
    tile = rows // 4
    z, y = me // 2, me % 2
    side = z // 2
    inner = (z + side) % 2
    at_z = {"a": 3 * side, "c": 1 + side, "g": 3 - 3 * side, "e": 2 - side}
    row = {k: 2 * v + y for k, v in at_z.items()}
    row.update({OVER_Y[k]: 2 * v + 1 - y for k, v in at_z.items()})

    loads = [
        pltpu.make_async_copy(
            feat_hbm.at[pl.ds(i * tile, tile)], feat.at[pl.ds(i * tile, tile)], lsem.at[i]
        )
        for i in range(4)
    ]
    loads.append(pltpu.make_async_copy(res_hbm, res, lsem.at[4]))
    loads.append(pltpu.make_async_copy(inv_hbm, inv, lsem.at[5]))
    for load in loads:
        load.start()
    barrier = pltpu.get_barrier_semaphore()
    z_near = 4 * side + 1 - z
    for target in ({"row": 2 * z + 1 - y}, {"row": 2 * z_near + y}, {"col": 1 - core}):
        pl.semaphore_signal(barrier, inc=1, device_id=target, device_id_type=MESH)

    @pl.when(inner == 1)
    def _():
        pl.semaphore_signal(barrier, inc=1, device_id={"row": row["e"]}, device_id_type=MESH)

    def message(item, link, target):
        r = row[item[1]]
        if item[0] == "X":
            p = int(item[2])
            ref = xall.at[r, pl.ds(p * quarter, quarter)]
            src, dst, send, recv = ref, ref, xs.at[link, r, p], xr.at[r, p]
        elif item[0] == "C":
            src, dst, send, recv = call.at[r], call.at[r], cs.at[link, r], cr.at[r]
        elif item[0] == "R":
            src, dst, send, recv = own.at[r], part.at[r], rs.at[r], rr.at[r]
        elif item[0] == "S":
            src, dst, send, recv = part.at[r], half_sum.at[r], ss.at[r], sr.at[r]
        else:
            src, dst, send, recv = own.at[r], col_sum.at[r], ts.at[r], tr.at[r]
        return pltpu.make_async_remote_copy(
            src_ref=src, dst_ref=dst, send_sem=send, recv_sem=recv, device_id={"row": row[target]},
            device_id_type=MESH,
        )

    base = me * rows

    def local(i):
        return jnp.maximum(jnp.minimum(ids[i] - base, rows - 1), 0)

    def gather_x(p):
        def body(i, _):
            i = p * quarter + i
            xall[me, pl.ds(i, 1), :] = feat[pl.ds(local(core * half + i), 1), :]
            return 0

        lax.fori_loop(0, quarter, body, 0, unroll=8)

    def gather_res():
        def body(i, _):
            change[pl.ds(i, 1), :] = res[pl.ds(local(i), 1), :]
            return 0

        lax.fori_loop(0, blk, body, 0, unroll=8)
        hi, lo = split(change[pl.ds(0, blk)])
        bres[0] = hi
        bres[1] = lo

    def partial_value(k):
        own[row[k]] = dot3(split(inv[row[k], 0]), (bres[0], bres[1]), NN)

    def split_feat():
        def body(i, _):
            at = pl.ds(pl.multiple_of(i * half, half), half)
            hi, lo = split(feat[at])
            fhi[at] = hi
            flo[at] = lo
            return 0

        lax.fori_loop(0, rows // half, body, 0)

    def load_x(chunks):
        for j, k in enumerate(chunks):
            hi, lo = split(xall[row[k]])
            xh[pl.ds(j * half, half)] = hi
            xl[pl.ds(j * half, half)] = lo

    def gram(slot, chunks, first, last):
        cols = len(chunks) * half
        to = pl.ds(slot * half, cols)

        def body(i, _):
            at = pl.ds(pl.multiple_of(i * tile, tile), tile)
            g = dot3((fhi[at], flo[at]), (xh[pl.ds(0, cols)], xl[pl.ds(0, cols)]), NT)
            g = g * (1.0 / feats) + 0.5
            hi, lo = split(g * g)
            khi[at, to] = hi
            klo[at, to] = lo
            return 0

        lax.fori_loop(first, last, body, 0)

    def load_c(chunks):
        for j, k in enumerate(chunks):
            hi, lo = split(call[row[k]])
            chi[pl.ds(j * half, half)] = hi
            clo[pl.ds(j * half, half)] = lo

    def product(slot, at):
        to = pl.ds(slot * half, blk)
        return dot3((khi[at, to], klo[at, to]), (chi[...], clo[...]), NN)

    def apply(slot, chunks, first):
        load_c(chunks)

        def body(i, _):
            at = pl.ds(pl.multiple_of(i * tile, tile), tile)
            add = product(slot, at)
            change[at] = add if first else change[at] + add
            return 0

        lax.fori_loop(0, 4, body, 0)

    mine = pl.ds(pl.multiple_of(core * width, width), width)
    theirs = pl.ds(pl.multiple_of((1 - core) * width, width), width)

    def swap(i):
        at = pl.ds(i * tile, tile)
        return pltpu.make_async_remote_copy(
            src_ref=change.at[at, theirs], dst_ref=ebuf.at[at], send_sem=es.at[i],
            recv_sem=er.at[i], device_id={"col": 1 - core}, device_id_type=MESH,
        )

    def finish(slot, chunks):
        load_c(chunks)
        for i in range(4):
            at = pl.ds(i * tile, tile)
            change[at] += product(slot, at)
            swap(i).start()
        for i in range(4):
            at = pl.ds(i * tile, tile)
            swap(i).wait_recv()
            out[at] = res[at, mine] - (change[at, mine] + ebuf[at])

    def run(is_inner, here, sends, arrivals, steps):
        queues = [[link, target, list(order)] for link, target, order in sends]
        have, sent = set(), []

        def issue():
            for link, target, order in queues:
                while order and order[0] in have:
                    item = order.pop(0)
                    copy = message(item, link, target)
                    copy.start()
                    sent.append(copy)

        for load in loads[:4]:
            load.wait()
        for p in range(4):
            gather_x(p)
            have.add(f"X{here}{p}")
            if p == 0:
                pl.semaphore_wait(barrier, 4 if is_inner else 3)
            issue()
        loads[4].wait()
        loads[5].wait()
        gather_res()
        for k in "fdhbgeac":
            partial_value(k)
            if not is_inner:
                have.add("R" + k)
                issue()
        split_feat()
        load_x(here)
        gram(*steps[0])

        def sums():
            for k in "efgh":
                if "S" + k not in have and "R" + k in have:
                    r = row[k]
                    part[r] = part[r] + own[r]
                    have.add("S" + k)
            for k in "bd":
                if "T" + k not in have and {"R" + k, "s" + k} <= have:
                    r = row[k]
                    own[r] = own[r] + part[r] + half_sum[r]
                    have.add("T" + k)
            for k in "ac":
                if "C" + k not in have and {"R" + k, "s" + k, "t" + k} <= have:
                    r = row[k]
                    call[r] = own[r] + part[r] + half_sum[r] + col_sum[r]
                    have.add("C" + k)

        for at, group in enumerate(arrivals):
            for item in group:
                message(item, 0, OVER_Y[here]).wait_recv()
                have.add(item if item[0] not in "ST" else item.lower())
                if is_inner:
                    sums()
                issue()
            for step in steps[1].get(at + 1, ()):
                step()
        assert not any(order for _, _, order in queues)
        for copy in sent:
            copy.wait_send()
        for i in range(4):
            swap(i).wait_send()

    def do(f, *args):
        return functools.partial(f, *args)

    @pl.when(inner == 0)
    def _():
        run(
            False, "a",
            ((1, "c", CORNER_Z), (0, "b", CORNER_Y)),
            slots(seen(CORNER_Y, OVER_Y), INNER_Z),
            (
                (0, "a", 0, 4),
                {
                    4: [do(load_x, "cb"), do(gram, 1, "cb", 0, 2)],
                    5: [do(gram, 1, "cb", 2, 4)],
                    9: [do(load_x, "ed"), do(gram, 5, "ed", 0, 2)],
                    10: [do(gram, 5, "ed", 2, 4)],
                    14: [do(load_x, "hg"), do(gram, 3, "hg", 0, 2)],
                    15: [do(gram, 3, "hg", 2, 4), do(apply, 0, "ac", True)],
                    16: [do(load_x, "f"), do(gram, 7, "f", 0, 4), do(apply, 4, "ge", False)],
                    17: [do(apply, 2, "bh", False)],
                    18: [do(finish, 6, "df")],
                },
            ),
        )

    @pl.when(inner == 1)
    def _():
        run(
            True, "c",
            ((1, "a", INNER_Z), (2, "e", INNER_W), (0, "d", INNER_Y)),
            slots(CORNER_Z, seen(INNER_W, OVER_Z), seen(INNER_Y, OVER_Y)),
            (
                (0, "c", 0, 4),
                {
                    6: [do(load_x, "ed"), do(gram, 6, "ed", 0, 2)],
                    7: [do(gram, 6, "ed", 2, 4)],
                    10: [do(load_x, "ag"), do(gram, 1, "ag", 0, 2)],
                    11: [do(gram, 1, "ag", 2, 4)],
                    12: [do(load_x, "h"), do(gram, 5, "h", 0, 4)],
                    13: [do(apply, 0, "ca", True)],
                    14: [do(apply, 6, "ed", False)],
                    16: [do(load_x, "bf"), do(gram, 3, "bf", 0, 4)],
                    17: [do(apply, 2, "gb", False)],
                    18: [do(finish, 4, "fh")],
                },
            ),
        )


def on_mesh(inverse, features, residual, block_ids):
    n, cores = lax.axis_size("row"), lax.axis_size("col")
    rows, feats = features.shape
    rhs = residual.shape[1]
    blk = block_ids.shape[0]
    half, tile = blk // cores, rows // 4
    any_spec = pl.BlockSpec(memory_space=pl.ANY)
    dma = pltpu.SemaphoreType.DMA
    return pl.pallas_call(
        mesh_kernel,
        out_shape=jax.ShapeDtypeStruct((rows, rhs // cores), F32),
        in_specs=[pl.BlockSpec(memory_space=pltpu.SMEM), any_spec, any_spec, any_spec],
        out_specs=pl.BlockSpec(memory_space=pltpu.VMEM),
        scratch_shapes=[
            pltpu.VMEM((rows, feats), F32),
            pltpu.VMEM((rows, feats), BF16),
            pltpu.VMEM((rows, feats), BF16),
            pltpu.VMEM((rows, rhs), F32),
            pltpu.VMEM(inverse.shape, F32),
            pltpu.VMEM((2, blk, rhs), BF16),
            pltpu.VMEM((n, half, feats), F32),
            pltpu.VMEM((blk, feats), BF16),
            pltpu.VMEM((blk, feats), BF16),
            pltpu.VMEM((rows, n * half), BF16),
            pltpu.VMEM((rows, n * half), BF16),
            pltpu.VMEM((n, half, rhs), F32),
            pltpu.VMEM((blk, rhs), BF16),
            pltpu.VMEM((blk, rhs), BF16),
            pltpu.VMEM((n, half, rhs), F32),
            pltpu.VMEM((n, half, rhs), F32),
            pltpu.VMEM((n, half, rhs), F32),
            pltpu.VMEM((n, half, rhs), F32),
            pltpu.VMEM((rows, rhs), F32),
            pltpu.VMEM((rows, rhs // cores), F32),
            dma((6,)),
            dma((3, n, 4)),
            dma((n, 4)),
            dma((3, n)),
            dma((n,)),
            dma((n,)),
            dma((n,)),
            dma((n,)),
            dma((n,)),
            dma((n,)),
            dma((n,)),
            dma((4,)),
            dma((4,)),
        ],
        compiler_params=pltpu.CompilerParams(
            collective_id=0, has_side_effects=True, vmem_limit_bytes=67043328
        ),
    )(block_ids, features, residual, inverse)


def two_lines(mesh):
    line = mesh.devices
    line = line[0, :, 0] if line.ndim == 3 else line.ravel()
    places = [getattr(d, "coords", None) for d in line]
    if any(p is None for p in places):
        return True
    return len({tuple(p)[:2] for p in places}) == 2


def solution(mesh):
    snake = two_lines(mesh)
    on_device = functools.partial(ring, snake)
    if snake and mesh.shape["row"] == len(OVER_Y):
        on_device = on_mesh
    return jax.shard_map(
        on_device,
        mesh=mesh,
        in_specs=(
            P("groups", "col", None, "row"),
            P(("groups", "row"), None),
            P(("groups", "row"), None),
            P(("groups", "row")),
        ),
        out_specs=P(("groups", "row"), "col"),
        check_vma=False,
    )
```

```python
import functools

import jax
import jax.numpy as jnp
from jax import lax
from jax.experimental import pallas as pl
from jax.experimental.pallas import tpu as pltpu
from jax.sharding import PartitionSpec as P

F32, BF16 = jnp.float32, jnp.bfloat16
MESH = pl.DeviceIdType.MESH
NN = (((1,), (0,)), ((), ()))
NT = (((1,), (1,)), ((), ()))


def split(v):
    hi = v.astype(BF16)
    return hi, (v - hi.astype(F32)).astype(BF16)


def dot3(a, b, dims):
    def one(x, y):
        return lax.dot_general(x, y, dims, preferred_element_type=F32)

    return one(a[0], b[1]) + one(a[1], b[0]) + one(a[0], b[0])


def ring_kernel(
    n, snake, ids, feat_hbm, res_hbm, inv_hbm, out, feat, fhi, flo, res, inv, bres, xh, xl, xbuf,
    kbuf, cbuf, rbuf, change, ebuf, lsem, xs_sem, xr_sem, ss_sem, sr_sem, es_sem, er_sem,
):
    me, core = lax.axis_index("row"), lax.axis_index("col")
    half_n = n // 2
    rows, feats = feat.shape
    blk = ids.shape[0]
    half = blk // 2
    quarter = half // 2
    width = out.shape[1]
    slots = kbuf.shape[0]
    tile = min(512, rows)

    def pos_of(r):
        if not snake:
            return r
        z, y = r // 2, r % 2
        return (1 - y) * z + y * (n - 1 - z)

    def row_of(p):
        p = lax.rem(p + n, n)
        if not snake:
            return p
        q = p // half_n
        return (1 - q) * 2 * p + q * (2 * (n - 1 - p) + 1)

    pos = pos_of(me)
    ahead = (row_of(pos + 1), row_of(pos + n - 1))
    sign = (1, -1)

    loads = [
        pltpu.make_async_copy(feat_hbm, feat, lsem.at[0]),
        pltpu.make_async_copy(res_hbm, res, lsem.at[1]),
        pltpu.make_async_copy(inv_hbm, inv, lsem.at[2]),
    ]
    for load in loads:
        load.start()
    barrier = pltpu.get_barrier_semaphore()
    for target in ({"row": ahead[0]}, {"row": ahead[1]}, {"col": 1 - core}):
        pl.semaphore_signal(barrier, inc=1, device_id=target, device_id_type=MESH)

    def remote(src, dst, send, recv, target):
        return pltpu.make_async_remote_copy(
            src_ref=src, dst_ref=dst, send_sem=send, recv_sem=recv, device_id=target,
            device_id_type=MESH,
        )

    def x_copy(way, p):
        d, h = p // 2 + 1, (p + way) % 2
        src = way * half + h * quarter
        dst = way * quarter if d == half_n else src
        return remote(
            xbuf.at[d - 1, pl.ds(src, quarter)], xbuf.at[d, pl.ds(dst, quarter)],
            xs_sem.at[way, p], xr_sem.at[way, p], {"row": ahead[way]},
        )

    def small_copy(way, m):
        if m <= half_n:
            at = pl.ds(way * quarter, quarter) if m == 1 else pl.ds(0, half)
            src, dst = rbuf.at[way, m - 1, at], rbuf.at[way, m, at]
        else:
            s = m - half_n
            if s == half_n:
                src = cbuf.at[s - 1, pl.ds(way * half + way * quarter, quarter)]
                dst = cbuf.at[s, pl.ds(way * quarter, quarter)]
            else:
                src = cbuf.at[s - 1, pl.ds(way * half, half)]
                dst = cbuf.at[s, pl.ds(way * half, half)]
        return remote(
            src, dst, ss_sem.at[way, m - 1], sr_sem.at[way, m - 1], {"row": ahead[way]}
        )

    def partial_value(owner, at=None):
        a = inv[owner, 0] if at is None else inv[owner, 0, at]
        return dot3(split(a), (bres[0], bres[1]), NN)

    def gram(d, cols):
        hi, lo = split(xbuf[d, pl.ds(0, cols)])
        xh[pl.ds(0, cols)] = hi
        xl[pl.ds(0, cols)] = lo

        def body(i, _):
            at = pl.ds(pl.multiple_of(i * tile, tile), tile)
            g = dot3((fhi[at], flo[at]), (xh[pl.ds(0, cols)], xl[pl.ds(0, cols)]), NT)
            g = g * (1.0 / feats) + 0.5
            kbuf[d % slots, at, pl.ds(0, cols)] = g * g
            return 0

        lax.fori_loop(0, rows // tile, body, 0)

    def apply(d, cols):
        c = split(cbuf[d, pl.ds(0, cols)])

        def body(i, _):
            at = pl.ds(pl.multiple_of(i * tile, tile), tile)
            add = dot3(split(kbuf[d % slots, at, pl.ds(0, cols)]), c, NN)
            change[at] = add if d == 0 else change[at] + add
            return 0

        lax.fori_loop(0, rows // tile, body, 0)

    base = me * rows

    def local(i):
        return jnp.maximum(jnp.minimum(ids[i] - base, rows - 1), 0)

    loads[0].wait()

    def gather_x(i, _):
        v = feat[pl.ds(local(core * half + i), 1), :]
        xbuf[0, pl.ds(i, 1), :] = v
        xbuf[0, pl.ds(half + i, 1), :] = v
        return 0

    lax.fori_loop(0, half, gather_x, 0, unroll=8)
    pl.semaphore_wait(barrier, 3)
    for way in (0, 1):
        x_copy(way, 0).start()

    loads[1].wait()

    def gather_res(i, _):
        change[pl.ds(i, 1), :] = res[pl.ds(local(i), 1), :]
        return 0

    lax.fori_loop(0, blk, gather_res, 0, unroll=8)
    hi, lo = split(change[pl.ds(0, blk)])
    bres[0] = hi
    bres[1] = lo
    loads[2].wait()
    for way in (0, 1):
        at = pl.ds(way * quarter, quarter)
        rbuf[way, 0, at] = partial_value(row_of(pos + half_n), at)
        small_copy(way, 1).start()

    def split_feat(i, _):
        at = pl.ds(pl.multiple_of(i * quarter, quarter), quarter)
        hi, lo = split(feat[at])
        fhi[at] = hi
        flo[at] = lo
        return 0

    lax.fori_loop(0, rows // quarter, split_feat, 0)
    for k in range(n):
        m = k + 1
        for way in (0, 1):
            small_copy(way, m).wait_recv()
            if m < half_n:
                part = partial_value(row_of(pos + n + sign[way] * (half_n - m)))
                if m == 1:
                    got, other = pl.ds(way * quarter, quarter), (1 - way) * quarter
                    lo_part, hi_part = part[:quarter], part[quarter:]
                    mine, rest = (lo_part, hi_part) if way == 0 else (hi_part, lo_part)
                    rbuf[way, 1, got] = rbuf[way, 1, got] + mine
                    rbuf[way, 1, pl.ds(other, quarter)] = rest
                else:
                    rbuf[way, m] = rbuf[way, m] + part
            elif m == half_n and way == 1:
                corr = partial_value(me) + rbuf[0, half_n] + rbuf[1, half_n]
                cbuf[0, pl.ds(0, half)] = corr
                cbuf[0, pl.ds(half, half)] = corr
                small_copy(0, m + 1).start()
            if m < n and (m != half_n or way == 1):
                small_copy(way, m + 1).start()
            if k >= 1:
                x_copy(way, k - 1).wait_recv()
            if k + 1 <= n - 2:
                x_copy(way, k + 1).start()
        if k == 0:
            gram(0, half)
        if k % 2 == 0 and k >= 2:
            gram(k // 2, blk)
        if k == half_n - 1:
            apply(0, half)
        if half_n <= k < n - 1:
            apply(k - half_n + 1, blk)

    gram(half_n, half)
    c = split(cbuf[half_n, pl.ds(0, half)])
    mine = pl.ds(pl.multiple_of(core * width, width), width)
    theirs = pl.ds(pl.multiple_of((1 - core) * width, width), width)
    step = tile // 2

    def swap(i):
        at = pl.ds(i * step, step)
        return remote(
            change.at[at, theirs], ebuf.at[at, pl.ds(0, width)], es_sem.at[i], er_sem.at[i],
            {"col": 1 - core},
        )

    for i in range(rows // step):
        at = pl.ds(i * step, step)
        change[at] += dot3(split(kbuf[half_n % slots, at, pl.ds(0, half)]), c, NN)
        swap(i).start()
    for i in range(rows // step):
        at = pl.ds(i * step, step)
        swap(i).wait_recv()
        out[at] = res[at, mine] - (change[at, mine] + ebuf[at, pl.ds(0, width)])
    for way in (0, 1):
        for p in range(n - 1):
            x_copy(way, p).wait_send()
        for m in range(1, n + 1):
            small_copy(way, m).wait_send()
    for i in range(rows // step):
        swap(i).wait_send()


def ring(snake, inverse, features, residual, block_ids):
    n, cores = lax.axis_size("row"), lax.axis_size("col")
    rows, feats = features.shape
    rhs = residual.shape[1]
    blk = block_ids.shape[0]
    half, half_n = blk // cores, n // 2
    any_spec = pl.BlockSpec(memory_space=pl.ANY)
    dma = pltpu.SemaphoreType.DMA
    tiles = rows // (min(512, rows) // 2)
    return pl.pallas_call(
        functools.partial(ring_kernel, n, snake),
        out_shape=jax.ShapeDtypeStruct((rows, rhs // cores), F32),
        in_specs=[pl.BlockSpec(memory_space=pltpu.SMEM), any_spec, any_spec, any_spec],
        out_specs=pl.BlockSpec(memory_space=pltpu.VMEM),
        scratch_shapes=[
            pltpu.VMEM((rows, feats), F32),
            pltpu.VMEM((rows, feats), BF16),
            pltpu.VMEM((rows, feats), BF16),
            pltpu.VMEM((rows, rhs), F32),
            pltpu.VMEM(inverse.shape, F32),
            pltpu.VMEM((2, blk, rhs), BF16),
            pltpu.VMEM((blk, feats), BF16),
            pltpu.VMEM((blk, feats), BF16),
            pltpu.VMEM((half_n + 1, blk, feats), F32),
            pltpu.VMEM((n // 4 + 2, rows, blk), F32),
            pltpu.VMEM((half_n + 1, blk, rhs), F32),
            pltpu.VMEM((2, half_n + 1, half, rhs), F32),
            pltpu.VMEM((rows, rhs), F32),
            pltpu.VMEM((rows, rhs), F32),
            dma((3,)),
            dma((2, n - 1)),
            dma((2, n - 1)),
            dma((2, n)),
            dma((2, n)),
            dma((tiles,)),
            dma((tiles,)),
        ],
        compiler_params=pltpu.CompilerParams(
            collective_id=0, has_side_effects=True, vmem_limit_bytes=67043328
        ),
    )(block_ids, features, residual, inverse)


CORNER_Z = (
    "Xa0", "Xa1", "Rf", "Rd", "Rh", "Rb", "Xa2", "Xa3", "Rg", "Re", "Ra", "Rc",
    "Xb0", "Xb1", "Xb2", "Xb3",
)
CORNER_Y = (
    "Xa0", "Xa2", "Xa3", "Xa1", "Xc0", "Xc1", "Xc2", "Xc3", "Xe0", "Xg0", "Xe1", "Xg1",
    "Xg2", "Xg3", "Xe2", "Xe3", "Cg", "Ce",
)
INNER_Z = (
    "Xc0", "Xc1", "Xc2", "Xc3", "Xe2", "Xe3", "Xe0", "Xg0", "Xe1", "Xg1", "Xg2", "Xg3",
    "Ca", "Cc", "Cg", "Ce", "Cb", "Cd",
)
INNER_W = (
    "Xc0", "Xc2", "Xc3", "Xc1", "Sf", "Xa0", "Sh", "Xa1", "Xa2", "Xa3", "Sg", "Se", "Ca", "Cc",
)
INNER_Y = (
    "Xc0", "Xc1", "Xc2", "Xe2", "Xe3", "Xc3", "Td", "Xg0", "Tb", "Xg1", "Xg2", "Xg3",
    "Ca", "Cc", "Xe0", "Xe1", "Cg", "Ce",
)
OVER_Y = dict(zip("abcdefgh", "badcfehg"))
OVER_Z = dict(zip("abcdefgh", "ghefcdab"))


def seen(order, swap):
    return [i[0] + swap.get(i[1], i[1]) + i[2:] for i in order]


def slots(*links):
    most = max(len(link) for link in links)
    return [[link[k] for link in links if k < len(link)] for k in range(most)]


def mesh_kernel(
    ids_hbm, feat_hbm, res_hbm, inv_hbm, out, ids, feat, fhi, flo, res, inv, bres, xall, xh, xl,
    khi, klo, call, chi, clo, own, part, half_sum, col_sum, change, ebuf, lsem, xs, xr, cs, cr, rs, rr, ss,
    sr, ts, tr, es, er,
):
    me, core = lax.axis_index("row"), lax.axis_index("col")
    rows, feats = feat.shape
    blk = ids.shape[0]
    half = blk // 2
    quarter = half // 4
    width = out.shape[1]
    tile = rows // 4
    z, y = me // 2, me % 2
    side = z // 2
    inner = (z + side) % 2
    at_z = {"a": 3 * side, "c": 1 + side, "g": 3 - 3 * side, "e": 2 - side}
    row = {k: 2 * v + y for k, v in at_z.items()}
    row.update({OVER_Y[k]: 2 * v + 1 - y for k, v in at_z.items()})

    loads = [
        pltpu.make_async_copy(
            feat_hbm.at[pl.ds(i * tile, tile)], feat.at[pl.ds(i * tile, tile)], lsem.at[i]
        )
        for i in range(4)
    ]
    loads.append(pltpu.make_async_copy(ids_hbm, ids, lsem.at[6]))
    loads.append(pltpu.make_async_copy(res_hbm, res, lsem.at[4]))
    loads.append(pltpu.make_async_copy(inv_hbm, inv, lsem.at[5]))
    for load in loads:
        load.start()
    barrier = pltpu.get_barrier_semaphore()
    z_near = 4 * side + 1 - z
    for target in ({"row": 2 * z + 1 - y}, {"row": 2 * z_near + y}, {"col": 1 - core}):
        pl.semaphore_signal(barrier, inc=1, device_id=target, device_id_type=MESH)

    @pl.when(inner == 1)
    def _():
        pl.semaphore_signal(barrier, inc=1, device_id={"row": row["e"]}, device_id_type=MESH)

    def message(item, link, target):
        r = row[item[1]]
        if item[0] == "X":
            p = int(item[2])
            ref = xall.at[r, pl.ds(p * quarter, quarter)]
            src, dst, send, recv = ref, ref, xs.at[link, r, p], xr.at[r, p]
        elif item[0] == "C":
            src, dst, send, recv = call.at[r], call.at[r], cs.at[link, r], cr.at[r]
        elif item[0] == "R":
            src, dst, send, recv = own.at[r], part.at[r], rs.at[r], rr.at[r]
        elif item[0] == "S":
            src, dst, send, recv = part.at[r], half_sum.at[r], ss.at[r], sr.at[r]
        else:
            src, dst, send, recv = own.at[r], col_sum.at[r], ts.at[r], tr.at[r]
        return pltpu.make_async_remote_copy(
            src_ref=src, dst_ref=dst, send_sem=send, recv_sem=recv, device_id={"row": row[target]},
            device_id_type=MESH,
        )

    base = me * rows

    def local(i):
        return jnp.maximum(jnp.minimum(ids[i] - base, rows - 1), 0)

    def gather_x(p):
        def body(i, _):
            i = p * quarter + i
            xall[me, pl.ds(i, 1), :] = feat[pl.ds(local(core * half + i), 1), :]
            return 0

        lax.fori_loop(0, quarter, body, 0, unroll=8)

    def gather_res():
        def body(i, _):
            change[pl.ds(i, 1), :] = res[pl.ds(local(i), 1), :]
            return 0

        lax.fori_loop(0, blk, body, 0, unroll=8)
        hi, lo = split(change[pl.ds(0, blk)])
        bres[0] = hi
        bres[1] = lo

    def partial_value(k):
        own[row[k]] = dot3(split(inv[row[k], 0]), (bres[0], bres[1]), NN)

    def split_feat():
        def body(i, _):
            at = pl.ds(pl.multiple_of(i * half, half), half)
            hi, lo = split(feat[at])
            fhi[at] = hi
            flo[at] = lo
            return 0

        lax.fori_loop(0, rows // half, body, 0)

    def load_x(chunks):
        for j, k in enumerate(chunks):
            hi, lo = split(xall[row[k]])
            xh[pl.ds(j * half, half)] = hi
            xl[pl.ds(j * half, half)] = lo

    def gram(slot, chunks, first, last):
        cols = len(chunks) * half
        to = pl.ds(slot * half, cols)

        def body(i, _):
            at = pl.ds(pl.multiple_of(i * tile, tile), tile)
            g = dot3((fhi[at], flo[at]), (xh[pl.ds(0, cols)], xl[pl.ds(0, cols)]), NT)
            g = g * (1.0 / feats) + 0.5
            hi, lo = split(g * g)
            khi[at, to] = hi
            klo[at, to] = lo
            return 0

        lax.fori_loop(first, last, body, 0)

    def load_c(chunks):
        for j, k in enumerate(chunks):
            hi, lo = split(call[row[k]])
            chi[pl.ds(j * half, half)] = hi
            clo[pl.ds(j * half, half)] = lo

    def product(slot, at):
        to = pl.ds(slot * half, blk)
        return dot3((khi[at, to], klo[at, to]), (chi[...], clo[...]), NN)

    def apply(slot, chunks, first):
        load_c(chunks)

        def body(i, _):
            at = pl.ds(pl.multiple_of(i * tile, tile), tile)
            add = product(slot, at)
            change[at] = add if first else change[at] + add
            return 0

        lax.fori_loop(0, 4, body, 0)

    mine = pl.ds(pl.multiple_of(core * width, width), width)
    theirs = pl.ds(pl.multiple_of((1 - core) * width, width), width)

    def swap(i):
        at = pl.ds(i * tile, tile)
        return pltpu.make_async_remote_copy(
            src_ref=change.at[at, theirs], dst_ref=ebuf.at[at], send_sem=es.at[i],
            recv_sem=er.at[i], device_id={"col": 1 - core}, device_id_type=MESH,
        )

    def finish(slot, chunks):
        load_c(chunks)
        for i in range(4):
            at = pl.ds(i * tile, tile)
            change[at] += product(slot, at)
            swap(i).start()
        for i in range(4):
            at = pl.ds(i * tile, tile)
            swap(i).wait_recv()
            out[at] = res[at, mine] - (change[at, mine] + ebuf[at])

    def run(is_inner, here, sends, arrivals, steps):
        queues = [[link, target, list(order)] for link, target, order in sends]
        have, sent = set(), []

        def issue():
            for link, target, order in queues:
                while order and order[0] in have:
                    item = order.pop(0)
                    copy = message(item, link, target)
                    copy.start()
                    sent.append(copy)

        for load in loads[:5]:
            load.wait()
        for p in range(4):
            gather_x(p)
            have.add(f"X{here}{p}")
            if p == 0:
                pl.semaphore_wait(barrier, 4 if is_inner else 3)
            issue()
        loads[5].wait()
        loads[6].wait()
        gather_res()
        for k in "fdhbgeac":
            partial_value(k)
            if not is_inner:
                have.add("R" + k)
                issue()
        split_feat()
        load_x(here)
        gram(*steps[0])

        def sums():
            for k in "efgh":
                if "S" + k not in have and "R" + k in have:
                    r = row[k]
                    part[r] = part[r] + own[r]
                    have.add("S" + k)
            for k in "bd":
                if "T" + k not in have and {"R" + k, "s" + k} <= have:
                    r = row[k]
                    own[r] = own[r] + part[r] + half_sum[r]
                    have.add("T" + k)
            for k in "ac":
                if "C" + k not in have and {"R" + k, "s" + k, "t" + k} <= have:
                    r = row[k]
                    call[r] = own[r] + part[r] + half_sum[r] + col_sum[r]
                    have.add("C" + k)

        for at, group in enumerate(arrivals):
            for item in group:
                message(item, 0, OVER_Y[here]).wait_recv()
                have.add(item if item[0] not in "ST" else item.lower())
                if is_inner:
                    sums()
                issue()
            for step in steps[1].get(at + 1, ()):
                step()
        assert not any(order for _, _, order in queues)
        for copy in sent:
            copy.wait_send()
        for i in range(4):
            swap(i).wait_send()

    def do(f, *args):
        return functools.partial(f, *args)

    @pl.when(inner == 0)
    def _():
        run(
            False, "a",
            ((1, "c", CORNER_Z), (0, "b", CORNER_Y)),
            slots(seen(CORNER_Y, OVER_Y), INNER_Z),
            (
                (0, "a", 0, 4),
                {
                    4: [do(load_x, "cb"), do(gram, 1, "cb", 0, 2)],
                    5: [do(gram, 1, "cb", 2, 4)],
                    9: [do(load_x, "ed"), do(gram, 5, "ed", 0, 2)],
                    10: [do(gram, 5, "ed", 2, 4)],
                    14: [do(load_x, "hg"), do(gram, 3, "hg", 0, 2)],
                    15: [do(gram, 3, "hg", 2, 4), do(apply, 0, "ac", True)],
                    16: [do(load_x, "f"), do(gram, 7, "f", 0, 4), do(apply, 4, "ge", False)],
                    17: [do(apply, 2, "bh", False)],
                    18: [do(finish, 6, "df")],
                },
            ),
        )

    @pl.when(inner == 1)
    def _():
        run(
            True, "c",
            ((1, "a", INNER_Z), (2, "e", INNER_W), (0, "d", INNER_Y)),
            slots(CORNER_Z, seen(INNER_W, OVER_Z), seen(INNER_Y, OVER_Y)),
            (
                (0, "c", 0, 4),
                {
                    6: [do(load_x, "ed"), do(gram, 6, "ed", 0, 2)],
                    7: [do(gram, 6, "ed", 2, 4)],
                    10: [do(load_x, "ag"), do(gram, 1, "ag", 0, 2)],
                    11: [do(gram, 1, "ag", 2, 4)],
                    12: [do(load_x, "h"), do(gram, 5, "h", 0, 4)],
                    13: [do(apply, 0, "ca", True)],
                    14: [do(apply, 6, "ed", False)],
                    16: [do(load_x, "bf"), do(gram, 3, "bf", 0, 4)],
                    17: [do(apply, 2, "gb", False)],
                    18: [do(finish, 4, "fh")],
                },
            ),
        )


def on_mesh(inverse, features, residual, block_ids):
    n, cores = lax.axis_size("row"), lax.axis_size("col")
    rows, feats = features.shape
    rhs = residual.shape[1]
    blk = block_ids.shape[0]
    half, tile = blk // cores, rows // 4
    hbm_spec = pl.BlockSpec(memory_space=pltpu.HBM)
    dma = pltpu.SemaphoreType.DMA
    args = [
        pltpu.with_memory_space_constraint(v, pltpu.HBM)
        for v in (block_ids, features, residual, inverse)
    ]
    return pl.pallas_call(
        mesh_kernel,
        out_shape=jax.ShapeDtypeStruct((rows, rhs // cores), F32),
        in_specs=[hbm_spec] * 4,
        out_specs=pl.BlockSpec(memory_space=pltpu.VMEM),
        scratch_shapes=[
            pltpu.SMEM(block_ids.shape, jnp.int32),
            pltpu.VMEM((rows, feats), F32),
            pltpu.VMEM((rows, feats), BF16),
            pltpu.VMEM((rows, feats), BF16),
            pltpu.VMEM((rows, rhs), F32),
            pltpu.VMEM(inverse.shape, F32),
            pltpu.VMEM((2, blk, rhs), BF16),
            pltpu.VMEM((n, half, feats), F32),
            pltpu.VMEM((blk, feats), BF16),
            pltpu.VMEM((blk, feats), BF16),
            pltpu.VMEM((rows, n * half), BF16),
            pltpu.VMEM((rows, n * half), BF16),
            pltpu.VMEM((n, half, rhs), F32),
            pltpu.VMEM((blk, rhs), BF16),
            pltpu.VMEM((blk, rhs), BF16),
            pltpu.VMEM((n, half, rhs), F32),
            pltpu.VMEM((n, half, rhs), F32),
            pltpu.VMEM((n, half, rhs), F32),
            pltpu.VMEM((n, half, rhs), F32),
            pltpu.VMEM((rows, rhs), F32),
            pltpu.VMEM((rows, rhs // cores), F32),
            dma((7,)),
            dma((3, n, 4)),
            dma((n, 4)),
            dma((3, n)),
            dma((n,)),
            dma((n,)),
            dma((n,)),
            dma((n,)),
            dma((n,)),
            dma((n,)),
            dma((n,)),
            dma((4,)),
            dma((4,)),
        ],
        compiler_params=pltpu.CompilerParams(
            collective_id=0, has_side_effects=True, vmem_limit_bytes=34 * 2**20
        ),
    )(*args)


def two_lines(mesh):
    line = mesh.devices
    line = line[0, :, 0] if line.ndim == 3 else line.ravel()
    places = [getattr(d, "coords", None) for d in line]
    if any(p is None for p in places):
        return True
    return len({tuple(p)[:2] for p in places}) == 2


def solution(mesh):
    snake = two_lines(mesh)
    on_device = functools.partial(ring, snake)
    if snake and mesh.shape["row"] == len(OVER_Y):
        on_device = on_mesh
    return jax.shard_map(
        on_device,
        mesh=mesh,
        in_specs=(
            P("groups", "col", None, "row"),
            P(("groups", "row"), None),
            P(("groups", "row"), None),
            P(("groups", "row")),
        ),
        out_specs=P(("groups", "row"), "col"),
        check_vma=False,
    )
```

```python
import functools

import jax
import jax.numpy as jnp
from jax import lax
from jax.experimental import pallas as pl
from jax.experimental.pallas import tpu as pltpu
from jax.sharding import PartitionSpec as P

F32, BF16 = jnp.float32, jnp.bfloat16
MESH = pl.DeviceIdType.MESH
NN = (((1,), (0,)), ((), ()))
NT = (((1,), (1,)), ((), ()))


def split(v):
    hi = v.astype(BF16)
    return hi, (v - hi.astype(F32)).astype(BF16)


def dot3(a, b, dims):
    def one(x, y):
        return lax.dot_general(x, y, dims, preferred_element_type=F32)

    return one(a[0], b[1]) + one(a[1], b[0]) + one(a[0], b[0])


def ring_kernel(
    n, snake, ids, feat_hbm, res_hbm, inv_hbm, out, feat, fhi, flo, res, inv, bres, xh, xl, xbuf,
    kbuf, cbuf, rbuf, change, ebuf, lsem, xs_sem, xr_sem, ss_sem, sr_sem, es_sem, er_sem,
):
    me, core = lax.axis_index("row"), lax.axis_index("col")
    half_n = n // 2
    rows, feats = feat.shape
    blk = ids.shape[0]
    half = blk // 2
    quarter = half // 2
    width = out.shape[1]
    slots = kbuf.shape[0]
    tile = min(512, rows)

    def pos_of(r):
        if not snake:
            return r
        z, y = r // 2, r % 2
        return (1 - y) * z + y * (n - 1 - z)

    def row_of(p):
        p = lax.rem(p + n, n)
        if not snake:
            return p
        q = p // half_n
        return (1 - q) * 2 * p + q * (2 * (n - 1 - p) + 1)

    pos = pos_of(me)
    ahead = (row_of(pos + 1), row_of(pos + n - 1))
    sign = (1, -1)

    loads = [
        pltpu.make_async_copy(feat_hbm, feat, lsem.at[0]),
        pltpu.make_async_copy(res_hbm, res, lsem.at[1]),
        pltpu.make_async_copy(inv_hbm, inv, lsem.at[2]),
    ]
    for load in loads:
        load.start()
    barrier = pltpu.get_barrier_semaphore()
    for target in ({"row": ahead[0]}, {"row": ahead[1]}, {"col": 1 - core}):
        pl.semaphore_signal(barrier, inc=1, device_id=target, device_id_type=MESH)

    def remote(src, dst, send, recv, target):
        return pltpu.make_async_remote_copy(
            src_ref=src, dst_ref=dst, send_sem=send, recv_sem=recv, device_id=target,
            device_id_type=MESH,
        )

    def x_copy(way, p):
        d, h = p // 2 + 1, (p + way) % 2
        src = way * half + h * quarter
        dst = way * quarter if d == half_n else src
        return remote(
            xbuf.at[d - 1, pl.ds(src, quarter)], xbuf.at[d, pl.ds(dst, quarter)],
            xs_sem.at[way, p], xr_sem.at[way, p], {"row": ahead[way]},
        )

    def small_copy(way, m):
        if m <= half_n:
            at = pl.ds(way * quarter, quarter) if m == 1 else pl.ds(0, half)
            src, dst = rbuf.at[way, m - 1, at], rbuf.at[way, m, at]
        else:
            s = m - half_n
            if s == half_n:
                src = cbuf.at[s - 1, pl.ds(way * half + way * quarter, quarter)]
                dst = cbuf.at[s, pl.ds(way * quarter, quarter)]
            else:
                src = cbuf.at[s - 1, pl.ds(way * half, half)]
                dst = cbuf.at[s, pl.ds(way * half, half)]
        return remote(
            src, dst, ss_sem.at[way, m - 1], sr_sem.at[way, m - 1], {"row": ahead[way]}
        )

    def partial_value(owner, at=None):
        a = inv[owner, 0] if at is None else inv[owner, 0, at]
        return dot3(split(a), (bres[0], bres[1]), NN)

    def gram(d, cols):
        hi, lo = split(xbuf[d, pl.ds(0, cols)])
        xh[pl.ds(0, cols)] = hi
        xl[pl.ds(0, cols)] = lo

        def body(i, _):
            at = pl.ds(pl.multiple_of(i * tile, tile), tile)
            g = dot3((fhi[at], flo[at]), (xh[pl.ds(0, cols)], xl[pl.ds(0, cols)]), NT)
            g = g * (1.0 / feats) + 0.5
            kbuf[d % slots, at, pl.ds(0, cols)] = g * g
            return 0

        lax.fori_loop(0, rows // tile, body, 0)

    def apply(d, cols):
        c = split(cbuf[d, pl.ds(0, cols)])

        def body(i, _):
            at = pl.ds(pl.multiple_of(i * tile, tile), tile)
            add = dot3(split(kbuf[d % slots, at, pl.ds(0, cols)]), c, NN)
            change[at] = add if d == 0 else change[at] + add
            return 0

        lax.fori_loop(0, rows // tile, body, 0)

    base = me * rows

    def local(i):
        return jnp.maximum(jnp.minimum(ids[i] - base, rows - 1), 0)

    loads[0].wait()

    def gather_x(i, _):
        v = feat[pl.ds(local(core * half + i), 1), :]
        xbuf[0, pl.ds(i, 1), :] = v
        xbuf[0, pl.ds(half + i, 1), :] = v
        return 0

    lax.fori_loop(0, half, gather_x, 0, unroll=8)
    pl.semaphore_wait(barrier, 3)
    for way in (0, 1):
        x_copy(way, 0).start()

    loads[1].wait()

    def gather_res(i, _):
        change[pl.ds(i, 1), :] = res[pl.ds(local(i), 1), :]
        return 0

    lax.fori_loop(0, blk, gather_res, 0, unroll=8)
    hi, lo = split(change[pl.ds(0, blk)])
    bres[0] = hi
    bres[1] = lo
    loads[2].wait()
    for way in (0, 1):
        at = pl.ds(way * quarter, quarter)
        rbuf[way, 0, at] = partial_value(row_of(pos + half_n), at)
        small_copy(way, 1).start()

    def split_feat(i, _):
        at = pl.ds(pl.multiple_of(i * quarter, quarter), quarter)
        hi, lo = split(feat[at])
        fhi[at] = hi
        flo[at] = lo
        return 0

    lax.fori_loop(0, rows // quarter, split_feat, 0)
    for k in range(n):
        m = k + 1
        for way in (0, 1):
            small_copy(way, m).wait_recv()
            if m < half_n:
                part = partial_value(row_of(pos + n + sign[way] * (half_n - m)))
                if m == 1:
                    got, other = pl.ds(way * quarter, quarter), (1 - way) * quarter
                    lo_part, hi_part = part[:quarter], part[quarter:]
                    mine, rest = (lo_part, hi_part) if way == 0 else (hi_part, lo_part)
                    rbuf[way, 1, got] = rbuf[way, 1, got] + mine
                    rbuf[way, 1, pl.ds(other, quarter)] = rest
                else:
                    rbuf[way, m] = rbuf[way, m] + part
            elif m == half_n and way == 1:
                corr = partial_value(me) + rbuf[0, half_n] + rbuf[1, half_n]
                cbuf[0, pl.ds(0, half)] = corr
                cbuf[0, pl.ds(half, half)] = corr
                small_copy(0, m + 1).start()
            if m < n and (m != half_n or way == 1):
                small_copy(way, m + 1).start()
            if k >= 1:
                x_copy(way, k - 1).wait_recv()
            if k + 1 <= n - 2:
                x_copy(way, k + 1).start()
        if k == 0:
            gram(0, half)
        if k % 2 == 0 and k >= 2:
            gram(k // 2, blk)
        if k == half_n - 1:
            apply(0, half)
        if half_n <= k < n - 1:
            apply(k - half_n + 1, blk)

    gram(half_n, half)
    c = split(cbuf[half_n, pl.ds(0, half)])
    mine = pl.ds(pl.multiple_of(core * width, width), width)
    theirs = pl.ds(pl.multiple_of((1 - core) * width, width), width)
    step = tile // 2

    def swap(i):
        at = pl.ds(i * step, step)
        return remote(
            change.at[at, theirs], ebuf.at[at, pl.ds(0, width)], es_sem.at[i], er_sem.at[i],
            {"col": 1 - core},
        )

    for i in range(rows // step):
        at = pl.ds(i * step, step)
        change[at] += dot3(split(kbuf[half_n % slots, at, pl.ds(0, half)]), c, NN)
        swap(i).start()
    for i in range(rows // step):
        at = pl.ds(i * step, step)
        swap(i).wait_recv()
        out[at] = res[at, mine] - (change[at, mine] + ebuf[at, pl.ds(0, width)])
    for way in (0, 1):
        for p in range(n - 1):
            x_copy(way, p).wait_send()
        for m in range(1, n + 1):
            small_copy(way, m).wait_send()
    for i in range(rows // step):
        swap(i).wait_send()


def ring(snake, inverse, features, residual, block_ids):
    n, cores = lax.axis_size("row"), lax.axis_size("col")
    rows, feats = features.shape
    rhs = residual.shape[1]
    blk = block_ids.shape[0]
    half, half_n = blk // cores, n // 2
    any_spec = pl.BlockSpec(memory_space=pl.ANY)
    dma = pltpu.SemaphoreType.DMA
    tiles = rows // (min(512, rows) // 2)
    return pl.pallas_call(
        functools.partial(ring_kernel, n, snake),
        out_shape=jax.ShapeDtypeStruct((rows, rhs // cores), F32),
        in_specs=[pl.BlockSpec(memory_space=pltpu.SMEM), any_spec, any_spec, any_spec],
        out_specs=pl.BlockSpec(memory_space=pltpu.VMEM),
        scratch_shapes=[
            pltpu.VMEM((rows, feats), F32),
            pltpu.VMEM((rows, feats), BF16),
            pltpu.VMEM((rows, feats), BF16),
            pltpu.VMEM((rows, rhs), F32),
            pltpu.VMEM(inverse.shape, F32),
            pltpu.VMEM((2, blk, rhs), BF16),
            pltpu.VMEM((blk, feats), BF16),
            pltpu.VMEM((blk, feats), BF16),
            pltpu.VMEM((half_n + 1, blk, feats), F32),
            pltpu.VMEM((n // 4 + 2, rows, blk), F32),
            pltpu.VMEM((half_n + 1, blk, rhs), F32),
            pltpu.VMEM((2, half_n + 1, half, rhs), F32),
            pltpu.VMEM((rows, rhs), F32),
            pltpu.VMEM((rows, rhs), F32),
            dma((3,)),
            dma((2, n - 1)),
            dma((2, n - 1)),
            dma((2, n)),
            dma((2, n)),
            dma((tiles,)),
            dma((tiles,)),
        ],
        compiler_params=pltpu.CompilerParams(
            collective_id=0, has_side_effects=True, vmem_limit_bytes=67043328
        ),
    )(block_ids, features, residual, inverse)


CORNER_Z = (
    "Xa0", "Xa1", "Rf", "Rd", "Rh", "Rb", "Xa2", "Xa3", "Rg", "Re", "Ra", "Rc",
    "Xb0", "Xb1", "Xb2", "Xb3",
)
CORNER_Y = (
    "Xa0", "Xa2", "Xa3", "Xa1", "Xc0", "Xc1", "Xc2", "Xc3", "Xe2", "Xe3", "Xe0", "Xe1",
    "Xg0", "Xg1", "Xg2", "Xg3", "Cg", "Ce",
)
INNER_Z = (
    "Xc0", "Xc1", "Xc2", "Xc3", "Xe2", "Xe3", "Xe0", "Xg0", "Xe1", "Xg1", "Xg2", "Xg3",
    "Ca", "Cc", "Cg", "Ce", "Cb", "Cd",
)
INNER_W = (
    "Xc0", "Xc2", "Xc3", "Xc1", "Sf", "Xa0", "Sh", "Xa1", "Xa2", "Xa3", "Sg", "Se", "Ca", "Cc",
)
INNER_Y = (
    "Xc0", "Xc1", "Xc2", "Xe2", "Xe3", "Xc3", "Td", "Xg0", "Tb", "Xg1", "Xg2", "Xg3",
    "Ca", "Cc", "Xe0", "Xe1", "Cg", "Ce",
)
OVER_Y = dict(zip("abcdefgh", "badcfehg"))
OVER_Z = dict(zip("abcdefgh", "ghefcdab"))


def seen(order, swap):
    return [i[0] + swap.get(i[1], i[1]) + i[2:] for i in order]


def slots(*links):
    most = max(len(link) for link in links)
    return [[link[k] for link in links if k < len(link)] for k in range(most)]


def mesh_kernel(
    ids_hbm, feat_hbm, res_hbm, inv_hbm, out, ids, feat, fhi, flo, res, inv, bres, xall, xh, xl,
    khi, klo, call, chi, clo, own, part, half_sum, col_sum, change, ebuf, lsem, xs, xr, cs, cr, rs, rr, ss,
    sr, ts, tr, es, er,
):
    me, core = lax.axis_index("row"), lax.axis_index("col")
    rows, feats = feat.shape
    blk = ids.shape[0]
    half = blk // 2
    quarter = half // 4
    width = out.shape[1]
    tile = rows // 4
    z, y = me // 2, me % 2
    side = z // 2
    inner = (z + side) % 2
    at_z = {"a": 3 * side, "c": 1 + side, "g": 3 - 3 * side, "e": 2 - side}
    row = {k: 2 * v + y for k, v in at_z.items()}
    row.update({OVER_Y[k]: 2 * v + 1 - y for k, v in at_z.items()})

    loads = [
        pltpu.make_async_copy(
            feat_hbm.at[pl.ds(i * tile, tile)], feat.at[pl.ds(i * tile, tile)], lsem.at[i]
        )
        for i in range(4)
    ]
    loads.append(pltpu.make_async_copy(ids_hbm, ids, lsem.at[6]))
    loads.append(pltpu.make_async_copy(res_hbm, res, lsem.at[4]))
    loads.append(pltpu.make_async_copy(inv_hbm, inv, lsem.at[5]))
    loads[4].start()
    for load in loads[:4] + loads[5:]:
        load.start()
    barrier = pltpu.get_barrier_semaphore()
    z_near = 4 * side + 1 - z
    for target in ({"row": 2 * z + 1 - y}, {"row": 2 * z_near + y}, {"col": 1 - core}):
        pl.semaphore_signal(barrier, inc=1, device_id=target, device_id_type=MESH)

    @pl.when(inner == 1)
    def _():
        pl.semaphore_signal(barrier, inc=1, device_id={"row": row["e"]}, device_id_type=MESH)

    def message(item, link, target):
        r = row[item[1]]
        if item[0] == "X":
            p = int(item[2])
            ref = xall.at[r, pl.ds(p * quarter, quarter)]
            src, dst, send, recv = ref, ref, xs.at[link, r, p], xr.at[r, p]
        elif item[0] == "C":
            src, dst, send, recv = call.at[r], call.at[r], cs.at[link, r], cr.at[r]
        elif item[0] == "R":
            src, dst, send, recv = own.at[r], part.at[r], rs.at[r], rr.at[r]
        elif item[0] == "S":
            src, dst, send, recv = part.at[r], half_sum.at[r], ss.at[r], sr.at[r]
        else:
            src, dst, send, recv = own.at[r], col_sum.at[r], ts.at[r], tr.at[r]
        return pltpu.make_async_remote_copy(
            src_ref=src, dst_ref=dst, send_sem=send, recv_sem=recv, device_id={"row": row[target]},
            device_id_type=MESH,
        )

    base = me * rows

    def local(i):
        return jnp.maximum(jnp.minimum(ids[i] - base, rows - 1), 0)

    def gather_x(p):
        def body(i, _):
            i = p * quarter + i
            xall[me, pl.ds(i, 1), :] = feat[pl.ds(local(core * half + i), 1), :]
            return 0

        lax.fori_loop(0, quarter, body, 0, unroll=8)

    def gather_res():
        def body(i, _):
            change[pl.ds(i, 1), :] = res[pl.ds(local(i), 1), :]
            return 0

        lax.fori_loop(0, blk, body, 0, unroll=8)
        hi, lo = split(change[pl.ds(0, blk)])
        bres[0] = hi
        bres[1] = lo

    def partial_value(k):
        own[row[k]] = dot3(split(inv[row[k], 0]), (bres[0], bres[1]), NN)

    def split_feat():
        def body(i, _):
            at = pl.ds(pl.multiple_of(i * half, half), half)
            hi, lo = split(feat[at])
            fhi[at] = hi
            flo[at] = lo
            return 0

        lax.fori_loop(0, rows // half, body, 0)

    def load_x(chunks):
        for j, k in enumerate(chunks):
            hi, lo = split(xall[row[k]])
            xh[pl.ds(j * half, half)] = hi
            xl[pl.ds(j * half, half)] = lo

    def gram(to, chunks, first, last):
        cols = len(chunks) * half

        def body(i, _):
            at = pl.ds(pl.multiple_of(i * tile, tile), tile)
            g = dot3((fhi[at], flo[at]), (xh[pl.ds(0, cols)], xl[pl.ds(0, cols)]), NT)
            g = g * (1.0 / feats) + 0.5
            hi, lo = split(g * g)
            for j, slot in enumerate(to):
                cut = slice(j * half, (j + 1) * half)
                khi[at, pl.ds(slot * half, half)] = hi[:, cut]
                klo[at, pl.ds(slot * half, half)] = lo[:, cut]
            return 0

        lax.fori_loop(first, last, body, 0)

    def load_c(chunks):
        for j, k in enumerate(chunks):
            hi, lo = split(call[row[k]])
            chi[pl.ds(j * half, half)] = hi
            clo[pl.ds(j * half, half)] = lo

    def product(slot, at):
        to = pl.ds(slot * half, blk)
        return dot3((khi[at, to], klo[at, to]), (chi[...], clo[...]), NN)

    def apply(slot, chunks, first):
        load_c(chunks)

        def body(i, _):
            at = pl.ds(pl.multiple_of(i * tile, tile), tile)
            add = product(slot, at)
            change[at] = add if first else change[at] + add
            return 0

        lax.fori_loop(0, 4, body, 0)

    mine = pl.ds(pl.multiple_of(core * width, width), width)
    theirs = pl.ds(pl.multiple_of((1 - core) * width, width), width)

    piece = rows // 1

    def swap(i):
        at = pl.ds(i * piece, piece)
        return pltpu.make_async_remote_copy(
            src_ref=change.at[at, theirs], dst_ref=ebuf.at[at], send_sem=es.at[i],
            recv_sem=er.at[i], device_id={"col": 1 - core}, device_id_type=MESH,
        )

    def finish(slot, chunks):
        load_c(chunks)
        for i in range(1):
            at = pl.ds(i * piece, piece)
            change[at] += product(slot, at)
            swap(i).start()
        for i in range(1):
            at = pl.ds(i * piece, piece)
            swap(i).wait_recv()
            out[at] = res[at, mine] - (change[at, mine] + ebuf[at])

    def run(is_inner, here, sends, arrivals, steps):
        queues = [[link, target, list(order)] for link, target, order in sends]
        have, sent = set(), []

        def issue():
            for link, target, order in queues:
                while order and order[0] in have:
                    item = order.pop(0)
                    copy = message(item, link, target)
                    copy.start()
                    sent.append(copy)

        for load in loads[:5]:
            load.wait()
        for p in range(4):
            gather_x(p)
            have.add(f"X{here}{p}")
            if p == 0:
                pl.semaphore_wait(barrier, 4 if is_inner else 3)
            issue()
        loads[5].wait()
        loads[6].wait()
        gather_res()
        for k in "fdhbgeac":
            partial_value(k)
            if not is_inner:
                have.add("R" + k)
                issue()
        split_feat()
        load_x(here)
        gram(*steps[0])

        def sums():
            for k in "efgh":
                if "S" + k not in have and "R" + k in have:
                    r = row[k]
                    part[r] = part[r] + own[r]
                    have.add("S" + k)
            for k in "bd":
                if "T" + k not in have and {"R" + k, "s" + k} <= have:
                    r = row[k]
                    own[r] = own[r] + part[r] + half_sum[r]
                    have.add("T" + k)
            for k in "ac":
                if "C" + k not in have and {"R" + k, "s" + k, "t" + k} <= have:
                    r = row[k]
                    call[r] = own[r] + part[r] + half_sum[r] + col_sum[r]
                    have.add("C" + k)

        for at, group in enumerate(arrivals):
            for item in group:
                message(item, 0, OVER_Y[here]).wait_recv()
                have.add(item if item[0] not in "ST" else item.lower())
                if is_inner:
                    sums()
                issue()
            for step in steps[1].get(at + 1, ()):
                step()
        assert not any(order for _, _, order in queues)
        for copy in sent:
            copy.wait_send()
        for i in range(1):
            swap(i).wait_send()

    def do(f, *args):
        return functools.partial(f, *args)

    @pl.when(inner == 0)
    def _():
        run(
            False, "a",
            ((1, "c", CORNER_Z), (0, "b", CORNER_Y)),
            slots(seen(CORNER_Y, OVER_Y), INNER_Z),
            (
                ((0,), "a", 0, 4),
                {
                    4: [do(load_x, "cb"), do(gram, (1, 4), "cb", 0, 2)],
                    5: [do(gram, (1, 4), "cb", 2, 4)],
                    9: [do(load_x, "ed"), do(gram, (3, 6), "ed", 0, 2)],
                    10: [do(gram, (3, 6), "ed", 2, 4)],
                    12: [do(load_x, "gf"), do(gram, (2, 7), "gf", 0, 2)],
                    13: [do(gram, (2, 7), "gf", 2, 4)],
                    14: [do(apply, 0, "ac", True)],
                    16: [do(load_x, "h"), do(gram, (5,), "h", 0, 4), do(apply, 2, "ge", False)],
                    17: [do(apply, 4, "bh", False)],
                    18: [do(finish, 6, "df")],
                },
            ),
        )

    @pl.when(inner == 1)
    def _():
        run(
            True, "c",
            ((1, "a", INNER_Z), (2, "e", INNER_W), (0, "d", INNER_Y)),
            slots(CORNER_Z, seen(INNER_W, OVER_Z), seen(INNER_Y, OVER_Y)),
            (
                ((0,), "c", 0, 4),
                {
                    6: [do(load_x, "ed"), do(gram, (4, 5), "ed", 0, 2)],
                    7: [do(gram, (4, 5), "ed", 2, 4)],
                    10: [do(load_x, "ag"), do(gram, (1, 7), "ag", 0, 2)],
                    11: [do(gram, (1, 7), "ag", 2, 4)],
                    12: [do(load_x, "h"), do(gram, (2,), "h", 0, 4)],
                    13: [do(apply, 0, "ca", True)],
                    14: [do(apply, 4, "ed", False)],
                    16: [do(load_x, "bf"), do(gram, (6, 3), "bf", 0, 4)],
                    17: [do(apply, 6, "bg", False)],
                    18: [do(finish, 2, "hf")],
                },
            ),
        )


def on_mesh(inverse, features, residual, block_ids):
    n, cores = lax.axis_size("row"), lax.axis_size("col")
    rows, feats = features.shape
    rhs = residual.shape[1]
    blk = block_ids.shape[0]
    half, tile = blk // cores, rows // 4
    hbm_spec = pl.BlockSpec(memory_space=pltpu.HBM)
    dma = pltpu.SemaphoreType.DMA
    args = [
        pltpu.with_memory_space_constraint(v, pltpu.HBM)
        for v in (block_ids, features, residual, inverse)
    ]
    return pl.pallas_call(
        mesh_kernel,
        out_shape=jax.ShapeDtypeStruct((rows, rhs // cores), F32),
        in_specs=[hbm_spec] * 4,
        out_specs=pl.BlockSpec(memory_space=pltpu.VMEM),
        scratch_shapes=[
            pltpu.SMEM(block_ids.shape, jnp.int32),
            pltpu.VMEM((rows, feats), F32),
            pltpu.VMEM((rows, feats), BF16),
            pltpu.VMEM((rows, feats), BF16),
            pltpu.VMEM((rows, rhs), F32),
            pltpu.VMEM(inverse.shape, F32),
            pltpu.VMEM((2, blk, rhs), BF16),
            pltpu.VMEM((n, half, feats), F32),
            pltpu.VMEM((blk, feats), BF16),
            pltpu.VMEM((blk, feats), BF16),
            pltpu.VMEM((rows, n * half), BF16),
            pltpu.VMEM((rows, n * half), BF16),
            pltpu.VMEM((n, half, rhs), F32),
            pltpu.VMEM((blk, rhs), BF16),
            pltpu.VMEM((blk, rhs), BF16),
            pltpu.VMEM((n, half, rhs), F32),
            pltpu.VMEM((n, half, rhs), F32),
            pltpu.VMEM((n, half, rhs), F32),
            pltpu.VMEM((n, half, rhs), F32),
            pltpu.VMEM((rows, rhs), F32),
            pltpu.VMEM((rows, rhs // cores), F32),
            dma((7,)),
            dma((3, n, 4)),
            dma((n, 4)),
            dma((3, n)),
            dma((n,)),
            dma((n,)),
            dma((n,)),
            dma((n,)),
            dma((n,)),
            dma((n,)),
            dma((n,)),
            dma((1,)),
            dma((1,)),
        ],
        compiler_params=pltpu.CompilerParams(
            collective_id=0, has_side_effects=True, vmem_limit_bytes=34 * 2**20
        ),
    )(*args)


def two_lines(mesh):
    line = mesh.devices
    line = line[0, :, 0] if line.ndim == 3 else line.ravel()
    places = [getattr(d, "coords", None) for d in line]
    if any(p is None for p in places):
        return True
    return len({tuple(p)[:2] for p in places}) == 2


def solution(mesh):
    snake = two_lines(mesh)
    on_device = functools.partial(ring, snake)
    if snake and mesh.shape["row"] == len(OVER_Y):
        on_device = on_mesh
    return jax.shard_map(
        on_device,
        mesh=mesh,
        in_specs=(
            P("groups", "col", None, "row"),
            P(("groups", "row"), None),
            P(("groups", "row"), None),
            P(("groups", "row")),
        ),
        out_specs=P(("groups", "row"), "col"),
        check_vma=False,
    )
```

```python
import functools

import jax
import jax.numpy as jnp
from jax import lax
from jax.experimental import pallas as pl
from jax.experimental.pallas import tpu as pltpu
from jax.sharding import PartitionSpec as P

F32, BF16 = jnp.float32, jnp.bfloat16
MESH = pl.DeviceIdType.MESH
NN = (((1,), (0,)), ((), ()))
NT = (((1,), (1,)), ((), ()))


def split(v):
    hi = v.astype(BF16)
    return hi, (v - hi.astype(F32)).astype(BF16)


def dot3(a, b, dims):
    def one(x, y):
        return lax.dot_general(x, y, dims, preferred_element_type=F32)

    return one(a[0], b[1]) + one(a[1], b[0]) + one(a[0], b[0])


def ring_kernel(
    n, snake, ids, feat_hbm, res_hbm, inv_hbm, out, feat, fhi, flo, res, inv, bres, xh, xl, xbuf,
    kbuf, cbuf, rbuf, change, ebuf, lsem, xs_sem, xr_sem, ss_sem, sr_sem, es_sem, er_sem,
):
    me, core = lax.axis_index("row"), lax.axis_index("col")
    half_n = n // 2
    rows, feats = feat.shape
    blk = ids.shape[0]
    half = blk // 2
    quarter = half // 2
    width = out.shape[1]
    slots = kbuf.shape[0]
    tile = min(512, rows)

    def pos_of(r):
        if not snake:
            return r
        z, y = r // 2, r % 2
        return (1 - y) * z + y * (n - 1 - z)

    def row_of(p):
        p = lax.rem(p + n, n)
        if not snake:
            return p
        q = p // half_n
        return (1 - q) * 2 * p + q * (2 * (n - 1 - p) + 1)

    pos = pos_of(me)
    ahead = (row_of(pos + 1), row_of(pos + n - 1))
    sign = (1, -1)

    loads = [
        pltpu.make_async_copy(feat_hbm, feat, lsem.at[0]),
        pltpu.make_async_copy(res_hbm, res, lsem.at[1]),
        pltpu.make_async_copy(inv_hbm, inv, lsem.at[2]),
    ]
    for load in loads:
        load.start()
    barrier = pltpu.get_barrier_semaphore()
    for target in ({"row": ahead[0]}, {"row": ahead[1]}, {"col": 1 - core}):
        pl.semaphore_signal(barrier, inc=1, device_id=target, device_id_type=MESH)

    def remote(src, dst, send, recv, target):
        return pltpu.make_async_remote_copy(
            src_ref=src, dst_ref=dst, send_sem=send, recv_sem=recv, device_id=target,
            device_id_type=MESH,
        )

    def x_copy(way, p):
        d, h = p // 2 + 1, (p + way) % 2
        src = way * half + h * quarter
        dst = way * quarter if d == half_n else src
        return remote(
            xbuf.at[d - 1, pl.ds(src, quarter)], xbuf.at[d, pl.ds(dst, quarter)],
            xs_sem.at[way, p], xr_sem.at[way, p], {"row": ahead[way]},
        )

    def small_copy(way, m):
        if m <= half_n:
            at = pl.ds(way * quarter, quarter) if m == 1 else pl.ds(0, half)
            src, dst = rbuf.at[way, m - 1, at], rbuf.at[way, m, at]
        else:
            s = m - half_n
            if s == half_n:
                src = cbuf.at[s - 1, pl.ds(way * half + way * quarter, quarter)]
                dst = cbuf.at[s, pl.ds(way * quarter, quarter)]
            else:
                src = cbuf.at[s - 1, pl.ds(way * half, half)]
                dst = cbuf.at[s, pl.ds(way * half, half)]
        return remote(
            src, dst, ss_sem.at[way, m - 1], sr_sem.at[way, m - 1], {"row": ahead[way]}
        )

    def partial_value(owner, at=None):
        a = inv[owner, 0] if at is None else inv[owner, 0, at]
        return dot3(split(a), (bres[0], bres[1]), NN)

    def gram(d, cols):
        hi, lo = split(xbuf[d, pl.ds(0, cols)])
        xh[pl.ds(0, cols)] = hi
        xl[pl.ds(0, cols)] = lo

        def body(i, _):
            at = pl.ds(pl.multiple_of(i * tile, tile), tile)
            g = dot3((fhi[at], flo[at]), (xh[pl.ds(0, cols)], xl[pl.ds(0, cols)]), NT)
            g = g * (1.0 / feats) + 0.5
            kbuf[d % slots, at, pl.ds(0, cols)] = g * g
            return 0

        lax.fori_loop(0, rows // tile, body, 0)

    def apply(d, cols):
        c = split(cbuf[d, pl.ds(0, cols)])

        def body(i, _):
            at = pl.ds(pl.multiple_of(i * tile, tile), tile)
            add = dot3(split(kbuf[d % slots, at, pl.ds(0, cols)]), c, NN)
            change[at] = add if d == 0 else change[at] + add
            return 0

        lax.fori_loop(0, rows // tile, body, 0)

    base = me * rows

    def local(i):
        return jnp.maximum(jnp.minimum(ids[i] - base, rows - 1), 0)

    loads[0].wait()

    def gather_x(i, _):
        v = feat[pl.ds(local(core * half + i), 1), :]
        xbuf[0, pl.ds(i, 1), :] = v
        xbuf[0, pl.ds(half + i, 1), :] = v
        return 0

    lax.fori_loop(0, half, gather_x, 0, unroll=8)
    pl.semaphore_wait(barrier, 3)
    for way in (0, 1):
        x_copy(way, 0).start()

    loads[1].wait()

    def gather_res(i, _):
        change[pl.ds(i, 1), :] = res[pl.ds(local(i), 1), :]
        return 0

    lax.fori_loop(0, blk, gather_res, 0, unroll=8)
    hi, lo = split(change[pl.ds(0, blk)])
    bres[0] = hi
    bres[1] = lo
    loads[2].wait()
    for way in (0, 1):
        at = pl.ds(way * quarter, quarter)
        rbuf[way, 0, at] = partial_value(row_of(pos + half_n), at)
        small_copy(way, 1).start()

    def split_feat(i, _):
        at = pl.ds(pl.multiple_of(i * quarter, quarter), quarter)
        hi, lo = split(feat[at])
        fhi[at] = hi
        flo[at] = lo
        return 0

    lax.fori_loop(0, rows // quarter, split_feat, 0)
    for k in range(n):
        m = k + 1
        for way in (0, 1):
            small_copy(way, m).wait_recv()
            if m < half_n:
                part = partial_value(row_of(pos + n + sign[way] * (half_n - m)))
                if m == 1:
                    got, other = pl.ds(way * quarter, quarter), (1 - way) * quarter
                    lo_part, hi_part = part[:quarter], part[quarter:]
                    mine, rest = (lo_part, hi_part) if way == 0 else (hi_part, lo_part)
                    rbuf[way, 1, got] = rbuf[way, 1, got] + mine
                    rbuf[way, 1, pl.ds(other, quarter)] = rest
                else:
                    rbuf[way, m] = rbuf[way, m] + part
            elif m == half_n and way == 1:
                corr = partial_value(me) + rbuf[0, half_n] + rbuf[1, half_n]
                cbuf[0, pl.ds(0, half)] = corr
                cbuf[0, pl.ds(half, half)] = corr
                small_copy(0, m + 1).start()
            if m < n and (m != half_n or way == 1):
                small_copy(way, m + 1).start()
            if k >= 1:
                x_copy(way, k - 1).wait_recv()
            if k + 1 <= n - 2:
                x_copy(way, k + 1).start()
        if k == 0:
            gram(0, half)
        if k % 2 == 0 and k >= 2:
            gram(k // 2, blk)
        if k == half_n - 1:
            apply(0, half)
        if half_n <= k < n - 1:
            apply(k - half_n + 1, blk)

    gram(half_n, half)
    c = split(cbuf[half_n, pl.ds(0, half)])
    mine = pl.ds(pl.multiple_of(core * width, width), width)
    theirs = pl.ds(pl.multiple_of((1 - core) * width, width), width)
    step = tile // 2

    def swap(i):
        at = pl.ds(i * step, step)
        return remote(
            change.at[at, theirs], ebuf.at[at, pl.ds(0, width)], es_sem.at[i], er_sem.at[i],
            {"col": 1 - core},
        )

    for i in range(rows // step):
        at = pl.ds(i * step, step)
        change[at] += dot3(split(kbuf[half_n % slots, at, pl.ds(0, half)]), c, NN)
        swap(i).start()
    for i in range(rows // step):
        at = pl.ds(i * step, step)
        swap(i).wait_recv()
        out[at] = res[at, mine] - (change[at, mine] + ebuf[at, pl.ds(0, width)])
    for way in (0, 1):
        for p in range(n - 1):
            x_copy(way, p).wait_send()
        for m in range(1, n + 1):
            small_copy(way, m).wait_send()
    for i in range(rows // step):
        swap(i).wait_send()


def ring(snake, inverse, features, residual, block_ids):
    n, cores = lax.axis_size("row"), lax.axis_size("col")
    rows, feats = features.shape
    rhs = residual.shape[1]
    blk = block_ids.shape[0]
    half, half_n = blk // cores, n // 2
    any_spec = pl.BlockSpec(memory_space=pl.ANY)
    dma = pltpu.SemaphoreType.DMA
    tiles = rows // (min(512, rows) // 2)
    return pl.pallas_call(
        functools.partial(ring_kernel, n, snake),
        out_shape=jax.ShapeDtypeStruct((rows, rhs // cores), F32),
        in_specs=[pl.BlockSpec(memory_space=pltpu.SMEM), any_spec, any_spec, any_spec],
        out_specs=pl.BlockSpec(memory_space=pltpu.VMEM),
        scratch_shapes=[
            pltpu.VMEM((rows, feats), F32),
            pltpu.VMEM((rows, feats), BF16),
            pltpu.VMEM((rows, feats), BF16),
            pltpu.VMEM((rows, rhs), F32),
            pltpu.VMEM(inverse.shape, F32),
            pltpu.VMEM((2, blk, rhs), BF16),
            pltpu.VMEM((blk, feats), BF16),
            pltpu.VMEM((blk, feats), BF16),
            pltpu.VMEM((half_n + 1, blk, feats), F32),
            pltpu.VMEM((n // 4 + 2, rows, blk), F32),
            pltpu.VMEM((half_n + 1, blk, rhs), F32),
            pltpu.VMEM((2, half_n + 1, half, rhs), F32),
            pltpu.VMEM((rows, rhs), F32),
            pltpu.VMEM((rows, rhs), F32),
            dma((3,)),
            dma((2, n - 1)),
            dma((2, n - 1)),
            dma((2, n)),
            dma((2, n)),
            dma((tiles,)),
            dma((tiles,)),
        ],
        compiler_params=pltpu.CompilerParams(
            collective_id=0, has_side_effects=True, vmem_limit_bytes=67043328
        ),
    )(block_ids, features, residual, inverse)


CORNER_Z = (
    "Xa0", "Xa1", "Rf", "Rd", "Rh", "Rb", "Xa2", "Xa3", "Rg", "Re", "Ra", "Rc",
    "Xb0", "Xb1", "Xb2", "Xb3",
)
CORNER_Y = (
    "Xa0", "Xa2", "Xa3", "Xa1", "Xc0", "Xc1", "Xc2", "Xc3", "Xe2", "Xe3", "Xe0", "Xe1",
    "Xg0", "Xg1", "Xg2", "Xg3", "Cg", "Ce",
)
INNER_Z = (
    "Xc0", "Xc1", "Xc2", "Xc3", "Xe2", "Xe3", "Xe0", "Xg0", "Xe1", "Xg1", "Xg2", "Xg3",
    "Ca", "Cc", "Cg", "Ce", "Cb", "Cd",
)
INNER_W = (
    "Xc0", "Xc2", "Xc3", "Xc1", "Sf", "Xa0", "Sh", "Xa1", "Xa2", "Xa3", "Sg", "Se", "Ca", "Cc",
)
INNER_Y = (
    "Xc0", "Xc1", "Xc2", "Xe2", "Xe3", "Xc3", "Td", "Xg0", "Tb", "Xg1", "Xg2", "Xg3",
    "Ca", "Cc", "Xe0", "Xe1", "Cg", "Ce",
)
OVER_Y = dict(zip("abcdefgh", "badcfehg"))
OVER_Z = dict(zip("abcdefgh", "ghefcdab"))


def seen(order, swap):
    return [i[0] + swap.get(i[1], i[1]) + i[2:] for i in order]


def slots(*links):
    most = max(len(link) for link in links)
    return [[link[k] for link in links if k < len(link)] for k in range(most)]


def mesh_kernel(
    ids_hbm, feat_hbm, res_hbm, inv_hbm, out, ids, feat0, feat1, feat2, feat3, fhi, flo, res, inv, bres, xall, xh, xl,
    khi, klo, call, chi, clo, own, part, half_sum, col_sum, change, ebuf, lsem, xs, xr, cs, cr, rs, rr, ss,
    sr, ts, tr, es, er,
):
    me, core = lax.axis_index("row"), lax.axis_index("col")
    feat = (feat0, feat1, feat2, feat3)
    rows, feats = fhi.shape
    blk = ids.shape[0]
    half = blk // 2
    quarter = half // 4
    width = out.shape[1]
    tile, strip = rows // 4, feats // 4
    z, y = me // 2, me % 2
    side = z // 2
    inner = (z + side) % 2
    at_z = {"a": 3 * side, "c": 1 + side, "g": 3 - 3 * side, "e": 2 - side}
    row = {k: 2 * v + y for k, v in at_z.items()}
    row.update({OVER_Y[k]: 2 * v + 1 - y for k, v in at_z.items()})

    loads = [
        pltpu.make_async_copy(
            feat_hbm.at[pl.ds(0, rows), pl.ds(i * strip, strip)],
            feat[i], lsem.at[i],
        )
        for i in range(4)
    ]
    loads.append(pltpu.make_async_copy(ids_hbm, ids, lsem.at[6]))
    loads.append(pltpu.make_async_copy(res_hbm, res, lsem.at[4]))
    loads.append(pltpu.make_async_copy(inv_hbm, inv, lsem.at[5]))
    for i in (4, 0, 1):
        loads[i].start()
    barrier = pltpu.get_barrier_semaphore()
    z_near = 4 * side + 1 - z
    for target in ({"row": 2 * z + 1 - y}, {"row": 2 * z_near + y}, {"col": 1 - core}):
        pl.semaphore_signal(barrier, inc=1, device_id=target, device_id_type=MESH)

    @pl.when(inner == 1)
    def _():
        pl.semaphore_signal(barrier, inc=1, device_id={"row": row["e"]}, device_id_type=MESH)

    def message(item, link, target, q=None):
        r = row[item[1]]
        if item[0] == "X":
            p = int(item[2])
            ref, p = xall.at[r, pl.ds(p * quarter, quarter)], p + 3
            if q is not None:
                ref, p = xall.at[r, pl.ds(0, quarter), pl.ds(q * strip, strip)], q
            src, dst, send, recv = ref, ref, xs.at[link, r, p], xr.at[r, p]
        elif item[0] == "C":
            src, dst, send, recv = call.at[r], call.at[r], cs.at[link, r], cr.at[r]
        elif item[0] == "R":
            src, dst, send, recv = own.at[r], part.at[r], rs.at[r], rr.at[r]
        elif item[0] == "S":
            src, dst, send, recv = part.at[r], half_sum.at[r], ss.at[r], sr.at[r]
        else:
            src, dst, send, recv = own.at[r], col_sum.at[r], ts.at[r], tr.at[r]
        return pltpu.make_async_remote_copy(
            src_ref=src, dst_ref=dst, send_sem=send, recv_sem=recv, device_id={"row": row[target]},
            device_id_type=MESH,
        )

    base = me * rows

    def local(i):
        return jnp.maximum(jnp.minimum(ids[i] - base, rows - 1), 0)

    def copies(item, link, target):
        pieces = range(4) if item[0] == "X" and item[2] == "0" else (None,)
        return [message(item, link, target, q) for q in pieces]

    def gather_x(p, strips):
        def body(i, _):
            i = p * quarter + i
            for q in strips:
                v = feat[q][pl.ds(local(core * half + i), 1), :]
                xall[me, pl.ds(i, 1), pl.ds(q * strip, strip)] = v
            return 0

        lax.fori_loop(0, quarter, body, 0, unroll=8)

    def gather_res():
        def body(i, _):
            change[pl.ds(i, 1), :] = res[pl.ds(local(i), 1), :]
            return 0

        lax.fori_loop(0, blk, body, 0, unroll=8)
        hi, lo = split(change[pl.ds(0, blk)])
        bres[0] = hi
        bres[1] = lo

    def partial_value(k):
        own[row[k]] = dot3(split(inv[row[k], 0]), (bres[0], bres[1]), NN)

    def split_feat():
        def body(i, _):
            at = pl.ds(pl.multiple_of(i * half, half), half)
            for q in range(4):
                hi, lo = split(feat[q][at])
                fhi[at, pl.ds(q * strip, strip)] = hi
                flo[at, pl.ds(q * strip, strip)] = lo
            return 0

        lax.fori_loop(0, rows // half, body, 0)

    def load_x(chunks):
        for j, k in enumerate(chunks):
            hi, lo = split(xall[row[k]])
            xh[pl.ds(j * half, half)] = hi
            xl[pl.ds(j * half, half)] = lo

    def gram(to, chunks, first, last):
        cols = len(chunks) * half

        def body(i, _):
            at = pl.ds(pl.multiple_of(i * tile, tile), tile)
            g = dot3((fhi[at], flo[at]), (xh[pl.ds(0, cols)], xl[pl.ds(0, cols)]), NT)
            g = g * (1.0 / feats) + 0.5
            hi, lo = split(g * g)
            for j, slot in enumerate(to):
                cut = slice(j * half, (j + 1) * half)
                khi[at, pl.ds(slot * half, half)] = hi[:, cut]
                klo[at, pl.ds(slot * half, half)] = lo[:, cut]
            return 0

        lax.fori_loop(first, last, body, 0)

    def load_c(chunks):
        for j, k in enumerate(chunks):
            hi, lo = split(call[row[k]])
            chi[pl.ds(j * half, half)] = hi
            clo[pl.ds(j * half, half)] = lo

    def product(slot, at):
        to = pl.ds(slot * half, blk)
        return dot3((khi[at, to], klo[at, to]), (chi[...], clo[...]), NN)

    def apply(slot, chunks, first):
        load_c(chunks)

        def body(i, _):
            at = pl.ds(pl.multiple_of(i * tile, tile), tile)
            add = product(slot, at)
            change[at] = add if first else change[at] + add
            return 0

        lax.fori_loop(0, 4, body, 0)

    mine = pl.ds(pl.multiple_of(core * width, width), width)
    theirs = pl.ds(pl.multiple_of((1 - core) * width, width), width)

    piece = rows // 1

    def swap(i):
        at = pl.ds(i * piece, piece)
        return pltpu.make_async_remote_copy(
            src_ref=change.at[at, theirs], dst_ref=ebuf.at[at], send_sem=es.at[i],
            recv_sem=er.at[i], device_id={"col": 1 - core}, device_id_type=MESH,
        )

    def finish(slot, chunks):
        load_c(chunks)
        for i in range(1):
            at = pl.ds(i * piece, piece)
            change[at] += product(slot, at)
            swap(i).start()
        for i in range(1):
            at = pl.ds(i * piece, piece)
            swap(i).wait_recv()
            out[at] = res[at, mine] - (change[at, mine] + ebuf[at])

    def run(is_inner, here, sends, arrivals, steps):
        queues = [[link, target, list(order)] for link, target, order in sends]
        have, sent = set(), []

        def issue():
            for link, target, order in queues:
                while order and order[0] in have:
                    item = order.pop(0)
                    for copy in copies(item, link, target):
                        copy.start()
                        sent.append(copy)

        loads[4].wait()
        for q in range(4):
            loads[q].wait()
            for i in {0: (2, 3), 1: (5, 6)}.get(q, ()):
                loads[i].start()
            gather_x(0, (q,))
            if q == 0:
                pl.semaphore_wait(barrier, 4 if is_inner else 3)
            for link, target, _ in queues:
                sent.append(message(f"X{here}0", link, target, q))
                sent[-1].start()
        for _, _, order in queues:
            assert order.pop(0) == f"X{here}0"
        have.add(f"X{here}0")
        for p in range(1, 4):
            gather_x(p, range(4))
            have.add(f"X{here}{p}")
            issue()
        loads[5].wait()
        loads[6].wait()
        gather_res()
        for k in "fdhbgeac":
            partial_value(k)
            if not is_inner:
                have.add("R" + k)
                issue()
        split_feat()
        load_x(here)
        gram(*steps[0])

        def sums():
            for k in "efgh":
                if "S" + k not in have and "R" + k in have:
                    r = row[k]
                    part[r] = part[r] + own[r]
                    have.add("S" + k)
            for k in "bd":
                if "T" + k not in have and {"R" + k, "s" + k} <= have:
                    r = row[k]
                    own[r] = own[r] + part[r] + half_sum[r]
                    have.add("T" + k)
            for k in "ac":
                if "C" + k not in have and {"R" + k, "s" + k, "t" + k} <= have:
                    r = row[k]
                    call[r] = own[r] + part[r] + half_sum[r] + col_sum[r]
                    have.add("C" + k)

        for at, group in enumerate(arrivals):
            for item in group:
                for copy in copies(item, 0, OVER_Y[here]):
                    copy.wait_recv()
                have.add(item if item[0] not in "ST" else item.lower())
                if is_inner:
                    sums()
                issue()
            for step in steps[1].get(at + 1, ()):
                step()
        assert not any(order for _, _, order in queues)
        for copy in sent:
            copy.wait_send()
        for i in range(1):
            swap(i).wait_send()

    def do(f, *args):
        return functools.partial(f, *args)

    @pl.when(inner == 0)
    def _():
        run(
            False, "a",
            ((1, "c", CORNER_Z), (0, "b", CORNER_Y)),
            slots(seen(CORNER_Y, OVER_Y), INNER_Z),
            (
                ((0,), "a", 0, 4),
                {
                    4: [do(load_x, "cb"), do(gram, (1, 4), "cb", 0, 2)],
                    5: [do(gram, (1, 4), "cb", 2, 4)],
                    9: [do(load_x, "ed"), do(gram, (3, 6), "ed", 0, 2)],
                    10: [do(gram, (3, 6), "ed", 2, 4)],
                    12: [do(load_x, "gf"), do(gram, (2, 7), "gf", 0, 2)],
                    13: [do(gram, (2, 7), "gf", 2, 4)],
                    14: [do(apply, 0, "ac", True)],
                    16: [do(load_x, "h"), do(gram, (5,), "h", 0, 4), do(apply, 2, "ge", False)],
                    17: [do(apply, 4, "bh", False)],
                    18: [do(finish, 6, "df")],
                },
            ),
        )

    @pl.when(inner == 1)
    def _():
        run(
            True, "c",
            ((1, "a", INNER_Z), (2, "e", INNER_W), (0, "d", INNER_Y)),
            slots(CORNER_Z, seen(INNER_W, OVER_Z), seen(INNER_Y, OVER_Y)),
            (
                ((0,), "c", 0, 4),
                {
                    6: [do(load_x, "ed"), do(gram, (4, 5), "ed", 0, 2)],
                    7: [do(gram, (4, 5), "ed", 2, 4)],
                    10: [do(load_x, "ag"), do(gram, (1, 7), "ag", 0, 2)],
                    11: [do(gram, (1, 7), "ag", 2, 4)],
                    12: [do(load_x, "h"), do(gram, (2,), "h", 0, 4)],
                    13: [do(apply, 0, "ca", True)],
                    14: [do(apply, 4, "ed", False)],
                    16: [do(load_x, "bf"), do(gram, (6, 3), "bf", 0, 4)],
                    17: [do(apply, 6, "bg", False)],
                    18: [do(finish, 2, "hf")],
                },
            ),
        )


def on_mesh(inverse, features, residual, block_ids):
    n, cores = lax.axis_size("row"), lax.axis_size("col")
    rows, feats = features.shape
    rhs = residual.shape[1]
    blk = block_ids.shape[0]
    half, tile = blk // cores, rows // 4
    hbm_spec = pl.BlockSpec(memory_space=pltpu.HBM)
    dma = pltpu.SemaphoreType.DMA
    args = [
        pltpu.with_memory_space_constraint(v, pltpu.HBM)
        for v in (block_ids, features, residual, inverse)
    ]
    return pl.pallas_call(
        mesh_kernel,
        out_shape=jax.ShapeDtypeStruct((rows, rhs // cores), F32),
        in_specs=[hbm_spec] * 4,
        out_specs=pl.BlockSpec(memory_space=pltpu.VMEM),
        scratch_shapes=[
            pltpu.SMEM(block_ids.shape, jnp.int32),
            pltpu.VMEM((rows, feats // 4), F32),
            pltpu.VMEM((rows, feats // 4), F32),
            pltpu.VMEM((rows, feats // 4), F32),
            pltpu.VMEM((rows, feats // 4), F32),
            pltpu.VMEM((rows, feats), BF16),
            pltpu.VMEM((rows, feats), BF16),
            pltpu.VMEM((rows, rhs), F32),
            pltpu.VMEM(inverse.shape, F32),
            pltpu.VMEM((2, blk, rhs), BF16),
            pltpu.VMEM((n, half, feats), F32),
            pltpu.VMEM((blk, feats), BF16),
            pltpu.VMEM((blk, feats), BF16),
            pltpu.VMEM((rows, n * half), BF16),
            pltpu.VMEM((rows, n * half), BF16),
            pltpu.VMEM((n, half, rhs), F32),
            pltpu.VMEM((blk, rhs), BF16),
            pltpu.VMEM((blk, rhs), BF16),
            pltpu.VMEM((n, half, rhs), F32),
            pltpu.VMEM((n, half, rhs), F32),
            pltpu.VMEM((n, half, rhs), F32),
            pltpu.VMEM((n, half, rhs), F32),
            pltpu.VMEM((rows, rhs), F32),
            pltpu.VMEM((rows, rhs // cores), F32),
            dma((7,)),
            dma((3, n, 7)),
            dma((n, 7)),
            dma((3, n)),
            dma((n,)),
            dma((n,)),
            dma((n,)),
            dma((n,)),
            dma((n,)),
            dma((n,)),
            dma((n,)),
            dma((1,)),
            dma((1,)),
        ],
        compiler_params=pltpu.CompilerParams(
            collective_id=0, has_side_effects=True, vmem_limit_bytes=34 * 2**20
        ),
    )(*args)


def two_lines(mesh):
    line = mesh.devices
    line = line[0, :, 0] if line.ndim == 3 else line.ravel()
    places = [getattr(d, "coords", None) for d in line]
    if any(p is None for p in places):
        return True
    return len({tuple(p)[:2] for p in places}) == 2


def solution(mesh):
    snake = two_lines(mesh)
    on_device = functools.partial(ring, snake)
    if snake and mesh.shape["row"] == len(OVER_Y):
        on_device = on_mesh
    return jax.shard_map(
        on_device,
        mesh=mesh,
        in_specs=(
            P("groups", "col", None, "row"),
            P(("groups", "row"), None),
            P(("groups", "row"), None),
            P(("groups", "row")),
        ),
        out_specs=P(("groups", "row"), "col"),
        check_vma=False,
    )
```
